32 devices in a mesh: grp: 2 (over x), ep: 16 (over z, y, core).
Axes of the slice: x: 2, y: 2, z: 4, core: 2. Of those that a mesh axis runs over, the one named last changes fastest.
Arguments:
- expert_ids: int32 [2048, 8], P(('grp', 'ep')), parts along dimension 0, may hold values from 0 to 15, all different within a row; in each aligned block of 64 rows (0 to 63, 64 to 127, ...) at most 64 rows name the same one
- route_gates: float32 [2048, 8], P(('grp', 'ep')), parts along dimension 0, may hold values from 0.1 to 0.5
- routed_in: bfloat16 [2048, 8, 2048], P(('grp', 'ep')), parts along dimension 0, may hold values from -6 to 6
- down_weight: bfloat16 [16, 1024, 3584], P('ep'), may hold values from -0.1875 to 0.1875
- slot_offset: int32 [1], replicated, may hold values from 0 to 15
Outputs:
- combined: bfloat16 [2048, 3584], P(('grp', 'ep')), parts along dimension 0
The draws below stay inside these ranges and needn't reach their ends.
There are 2 independent parts, one for each index of `grp`. The reference program is written for one: setup_inputs(seed, part) draws one part's arguments, and reference() takes and returns one part's arrays. A program takes and returns all parts, laid end to end along the dimension named above; an argument that names none is the same for every part. Nothing has to cross between parts.
Inputs may be any that keep to these rules, and one draw needn't show every extreme that they name: `expert_ids`: each row names 8 different experts. Among the tokens of one ep device, no expert is named by more than 64 tokens, a bound that some block reaches in some devices.
All inputs are finite; a program needn't handle non-finite values.
Results may differ from the reference program's by a relative error of at most 0.0057.
Values may be sent and summed in bfloat16 or wider, within the bound.
A program may use at most 128 MiB of HBM per device.

```python
import math
import jax
import jax.numpy as jnp
import numpy as np
from jax import lax

D = 3584
F = 1024
TOP = 8
TOK_DEV = 64
EXPERTS = 16
TOKENS = 1024
CAP = 64


def levels(stream_key, extent, split, smallest, largest):
    loudness = 1.0
    for dim, blocks in split:
        heights = jax.random.uniform(jax.random.fold_in(jax.random.fold_in(stream_key, 6), dim), (blocks,), jnp.float32, smallest / len(split), largest / len(split))
        loudness = loudness * jnp.repeat(jnp.exp(heights), extent[dim] // blocks).reshape((-1,) + (1,) * (len(extent) - 1 - dim))
    return loudness


def routed_block(rng, own, number, rows, amount, top, most, lean):
    ranking = jax.random.permutation(rng, amount)
    crowded, ordinary = portions_of(amount, rows * top, most, lean, True), portions_of(amount, rows * top, most, lean, False)
    places = jnp.arange(amount)

    def named(sizes, turn):
        used = int((sizes > 0).sum())
        fixed = max(1, used // 4)
        moved = fixed + (places - fixed + turn * (used - fixed)) % max(1, amount - fixed)
        return jnp.zeros((amount,), jnp.int32).at[ranking[jnp.where(places < fixed, places, moved)]].set(jnp.asarray(sizes, jnp.int32))

    sizes = jnp.where(number % 4 == 0, named(crowded, number // 4), named(ordinary, number - number // 4 - 1))
    mixed = jax.random.permutation(jax.random.fold_in(own, 3), amount)
    giver, taker = mixed[0:amount // 2 * 2:2], mixed[1:amount // 2 * 2:2]
    margin = jnp.minimum(sizes[giver] - 1, most - sizes[taker]) // 2
    margin = jnp.where((giver == ranking[0]) | (taker == ranking[0]) | (sizes[taker] == 0), 0, jnp.maximum(margin, 0))
    moved = jax.random.randint(jax.random.fold_in(own, 4), (amount // 2,), 0, 1 << 20) % (margin + 1)
    sizes = sizes.at[giver].add(-moved).at[taker].add(moved)
    members = jnp.searchsorted(jnp.cumsum(sizes), jnp.arange(rows * top), side="right").astype(jnp.int32)
    grid = members.reshape(top, rows).T
    grid = grid[jax.random.permutation(jax.random.fold_in(own, 1), rows)]
    turn = jax.random.randint(jax.random.fold_in(own, 2), (rows, 1), 0, top)
    return jnp.take_along_axis(grid, (jnp.arange(top)[None, :] + turn) % top, axis=1)


def portions_of(number_of, total, reach, lean, full):
    portions = [(1 << 20) // math.isqrt(rank ** lean) + 1 for rank in range(1, number_of + 1)]
    largest = reach if full else min(reach, max(-(-total // number_of), total * portions[0] // sum(portions)))
    least = 1 if total - largest >= number_of - 1 else 0
    counts, rest = [largest] + [least] * (number_of - 1), total - largest - least * (number_of - 1)
    while rest > 0:
        movable = [i for i in range(1, number_of) if counts[i] < largest] or [i for i in range(1, number_of) if counts[i] < reach]
        pool, budget = sum([portions[i] for i in movable]), rest
        for i in movable:
            more = min(reach - counts[i], max(1, budget * portions[i] // pool), rest)
            counts[i] = counts[i] + more
            rest = rest - more
    return np.array(counts)


def scatter_about(stream_key, shape, spread, bound, pieces=(), kind=jnp.bfloat16):
    values = jax.random.normal(stream_key, shape, jnp.float32) * spread
    if len(pieces) > 0:
        values = levels(stream_key, shape, pieces, -0.22, 0.18) * values
    return jnp.clip(values, min=-bound, max=bound).astype(kind)


def setup_inputs(seed: int = 0, part: int = 0) -> dict:
    splits = jax.random.split(jax.random.key(seed), 6)
    part_keys = jax.random.split(jax.random.fold_in(splits[5], part), 6)
    expert_ids_keys = jax.random.split(jax.random.fold_in(part_keys[0], 1), TOKENS // TOK_DEV)
    expert_ids_turns = jax.random.permutation(jax.random.fold_in(part_keys[0], 3), TOKENS // TOK_DEV)
    expert_ids = jax.vmap(lambda own, number: routed_block(jax.random.fold_in(part_keys[0], 2), own, number, TOK_DEV, EXPERTS, TOP, CAP, 2))(expert_ids_keys, expert_ids_turns).reshape((TOKENS, TOP))
    route_gates = jnp.clip(0.1 + 0.4 * jax.random.uniform(part_keys[1], (TOKENS, TOP), jnp.float32) ** levels(part_keys[1], (TOKENS, TOP), ((0, 16),), -0.2, 0.2), 0.1, 0.5)
    routed_in = scatter_about(part_keys[2], (TOKENS, TOP, 2 * F), 1.0, 6.0, ((0, 16),))
    down_weight = scatter_about(splits[3], (EXPERTS, F, D), F ** -0.5, 0.1875, ((0, 16),))
    slot_offset = jax.random.randint(splits[4], (1,), 0, EXPERTS).astype(jnp.int32)
    return dict(expert_ids=expert_ids, route_gates=route_gates, routed_in=routed_in, down_weight=down_weight, slot_offset=slot_offset)


def swiglu(packed):
    half = packed.shape[-1] // 2
    gate = packed[..., :half].astype(jnp.float32)
    upper = packed[..., half:].astype(jnp.float32)
    return (jax.nn.silu(gate) * upper).astype(jnp.bfloat16)


def reference(expert_ids, route_gates, routed_in, down_weight, slot_offset):
    pairs = expert_ids.reshape(-1).astype(jnp.int32)
    pair_count = pairs.shape[0]
    most_rows = EXPERTS * CAP
    hidden = swiglu(routed_in).reshape(pair_count, F)
    order = jnp.argsort(pairs, stable=True).astype(jnp.int32)
    inverse = jnp.argsort(order, stable=True).astype(jnp.int32)
    sorted_hidden = jnp.concatenate([hidden[order], jnp.zeros((most_rows, F), jnp.bfloat16)], axis=0)
    loads = jnp.sum((pairs[:, None] == jnp.arange(EXPERTS, dtype=jnp.int32)[None, :]).astype(jnp.int32), axis=0)
    starts = (jnp.cumsum(loads) - loads).astype(jnp.int32)

    def one_expert(carry, expert):
        start = starts[expert]
        rows = lax.dynamic_slice_in_dim(sorted_hidden, start, most_rows, 0)
        matrix = down_weight[jnp.mod(expert - slot_offset[0], EXPERTS).astype(jnp.int32)]
        result = jnp.dot(rows, matrix, preferred_element_type=jnp.float32).astype(jnp.bfloat16)
        live = jnp.arange(most_rows, dtype=jnp.int32) < loads[expert]
        before = lax.dynamic_slice_in_dim(carry, start, most_rows, 0)
        update = jnp.where(live[:, None], result, before)
        return lax.dynamic_update_slice_in_dim(carry, update, start, 0), None

    initial = jnp.zeros((pair_count + most_rows, D), jnp.bfloat16)
    filled, unused = lax.scan(one_expert, initial, jnp.arange(EXPERTS, dtype=jnp.int32))
    outputs = filled[:pair_count][inverse].reshape(TOKENS, TOP, D)
    total = jnp.zeros((TOKENS, D), jnp.float32)
    for choice_index in range(TOP):
        total = total + route_gates[:, choice_index, None] * outputs[:, choice_index].astype(jnp.float32)
    return total.astype(jnp.bfloat16)
```

```python
import functools

import jax
import jax.numpy as jnp
from jax import lax
from jax.experimental import pallas as pl
from jax.experimental.pallas import tpu as pltpu
from jax.sharding import PartitionSpec as P

MESH = pl.DeviceIdType.MESH
TILE = 256
COLUMNS = 896
PART = 8
LEAD = 2
LAG = 2
VMEM_LIMIT = 63 * 1024 * 1024


def swiglu(packed):
    half = packed.shape[-1] // 2
    gate = packed[..., :half].astype(jnp.float32)
    upper = packed[..., half:].astype(jnp.float32)
    return (jax.nn.silu(gate) * upper).astype(jnp.bfloat16)


def exchange_form(expert_ids, route_gates, routed_in, down_weight, slot_offset):
    experts = lax.axis_size("ep")
    tokens_here, chosen = expert_ids.shape
    pair_count = tokens_here * chosen
    capacity = 2 * pair_count // experts
    matrix = down_weight[0]
    offset = slot_offset[0]
    target = jnp.mod(expert_ids.reshape(pair_count) - offset, experts)
    onehot = (target[:, None] == jnp.arange(experts, dtype=jnp.int32)[None, :]).astype(jnp.int32)
    earlier = jnp.cumsum(onehot, axis=0) - onehot
    rank = jnp.sum(earlier * onehot, axis=1)
    row_index = target * capacity + rank
    source = (
        jnp.full((experts * capacity,), pair_count, jnp.int32)
        .at[row_index]
        .set(jnp.arange(pair_count, dtype=jnp.int32))
    )
    payload = swiglu(routed_in.reshape(pair_count, routed_in.shape[2]))
    padded = jnp.concatenate([payload, jnp.zeros((1, payload.shape[1]), jnp.bfloat16)], axis=0)
    outgoing = jnp.take(padded, source, axis=0).reshape(experts, capacity, payload.shape[1])
    results = jnp.einsum(
        "nkf,fd->nkd",
        lax.all_to_all(outgoing, "ep", split_axis=0, concat_axis=0, tiled=True),
        matrix,
        preferred_element_type=jnp.float32,
    ).astype(jnp.bfloat16)
    returned = lax.all_to_all(results, "ep", split_axis=0, concat_axis=0, tiled=True)
    width = returned.shape[2]
    picked = jnp.take(returned.reshape(experts * capacity, width), row_index, axis=0).reshape(
        tokens_here, chosen, width
    )
    total = jnp.zeros((tokens_here, width), jnp.float32)
    for choice_index in range(chosen):
        total = total + route_gates[:, choice_index, None] * picked[:, choice_index].astype(
            jnp.float32
        )
    return total.astype(jnp.bfloat16)


def flipped(index, distance):
    result, bit = index, 1
    while bit <= distance:
        if distance & bit:
            result = result + bit - 2 * bit * lax.rem(lax.div(index, bit), 2)
        bit *= 2
    return result


def slot_distance(n, slot):
    groups = n // 4
    return (groups - 1 - slot % groups) * 4 + (slot // groups % 2) * 2 + slot // (2 * groups)


def kernel(
    n,
    offset_ref,
    ids_ref,
    gate_ref,
    x_hbm,
    w_hbm,
    out_ref,
    x,
    w,
    outg,
    recv,
    lhs,
    own,
    psend,
    crecv,
    ysend,
    yrecv,
    zsend,
    zrecv,
    wsem,
    xsem,
    dsend_sem,
    drecv_sem,
    csend_sem,
    crecv_sem,
    ysend_sem,
    yrecv_sem,
    zsend_sem,
    zrecv_sem,
):
    me = lax.axis_index("ep")
    features, width = w.shape
    chunks, _, part, _ = recv.shape
    chosen = ids_ref.shape[0]
    pairs = part * chosen
    rows_all = n * part
    groups = n // 4
    half = n // 2
    line_at = me // 4
    at_end = jnp.logical_or(line_at == 0, line_at == groups - 1)

    def remote(src, dst, send_sem, recv_sem, distance):
        return pltpu.make_async_remote_copy(
            src_ref=src,
            dst_ref=dst,
            send_sem=send_sem,
            recv_sem=recv_sem,
            device_id={"ep": flipped(me, distance)},
            device_id_type=MESH,
        )

    def send(*args):
        copy = remote(*args)
        copy.start()
        return copy

    barrier = pltpu.get_barrier_semaphore()
    for d in range(1, n):
        pl.semaphore_signal(barrier, inc=1, device_id={"ep": flipped(me, d)}, device_id_type=MESH)
    x_copies = []
    for k in range(chunks):
        tokens_of = pl.ds(k * part, part)
        x_copies.append(pltpu.make_async_copy(x_hbm.at[tokens_of], x.at[tokens_of], xsem.at[k]))
        x_copies[k].start()
    w_copy = pltpu.make_async_copy(w_hbm.at[0], w, wsem.at[0])
    w_copy.start()

    slots = [slot_distance(n, s) for s in range(n)]
    peers = [flipped(me, d) for d in slots]
    target_all = lax.rem(ids_ref[...] - offset_ref[0] + n, n).astype(jnp.float32).T
    gates_all = gate_ref[...].T
    lane = lax.broadcasted_iota(jnp.int32, (chosen, pairs), 1)
    spread = (lane % chosen == lax.broadcasted_iota(jnp.int32, (chosen, pairs), 0)).astype(jnp.bfloat16)
    mine = (
        lax.broadcasted_iota(jnp.int32, (rows_all, pairs), 1) // chosen
        == lax.broadcasted_iota(jnp.int32, (rows_all, pairs), 0) % part
    )
    peer_of = jnp.concatenate([jnp.full((part, chosen), e, jnp.int32) for e in peers], axis=0).astype(
        jnp.float32
    )

    dispatch = {}
    for k in range(chunks):
        for s, d in enumerate(slots):
            if d:
                dispatch[k, d] = remote(
                    outg.at[k, s], recv.at[k, s], dsend_sem.at[k, s], drecv_sem.at[k, s], d
                )

    def issue(k, lines):
        if k < chunks:
            for dz in lines:
                for low in (2, 3, 0, 1):
                    if dz * 4 + low:
                        dispatch[k, dz * 4 + low].start()

    near, far = (0, 1), tuple(range(groups - 1, 1, -1))

    def issue_early(k):
        issue(k, (0,))

        @pl.when(jnp.logical_not(at_end))
        def _():
            issue(k, far + (1,))

        @pl.when(at_end)
        def _():
            if k < LEAD + 2:
                issue(k, (1,))
            if 0 < k <= LEAD:
                issue(k - 1, far)

    def issue_late(k):
        @pl.when(at_end)
        def _():
            issue(k + LEAD + 2, (1,))
            issue(k + LEAD, far)

    for k in range(chunks):
        target = target_all[k * part : (k + 1) * part]
        gates = gates_all[k * part : (k + 1) * part]
        hit = jnp.where(jnp.concatenate([target] * n, axis=0) == peer_of, 1.0, 0.0)
        scale = jnp.sum(hit * jnp.concatenate([gates] * n, axis=0), axis=1, keepdims=True)
        wanted = jnp.dot(hit.astype(jnp.bfloat16), spread, preferred_element_type=jnp.float32)
        pick = jnp.where(mine, wanted, 0.0).astype(jnp.bfloat16)
        x_copies[k].wait()
        for c in range(0, features, TILE):
            gate = x[k * part : (k + 1) * part, :, c : c + TILE].astype(jnp.float32)
            upper = x[k * part : (k + 1) * part, :, features + c : features + c + TILE].astype(jnp.float32)
            hidden = (jax.nn.silu(gate) * upper).reshape(pairs, TILE).astype(jnp.bfloat16)
            rows = jnp.dot(pick, hidden, preferred_element_type=jnp.float32)
            rows = (rows * scale).reshape(n, part, TILE).astype(jnp.bfloat16)
            for s, d in enumerate(slots):
                if d:
                    outg[k, s, :, c : c + TILE] = rows[s]
                else:
                    recv[k, s, :, c : c + TILE] = rows[s]
        if k == 0:
            pl.semaphore_wait(barrier, n - 1)
        issue_early(k)
    w_copy.wait()

    core, side, line = {}, {}, {}
    halves = 2
    span = width // halves

    def multiply(k):
        for d in slots:
            if d:
                dispatch[k, d].wait_recv()
        issue_late(k)
        lhs[...] = recv[k].astype(jnp.float32).reshape(rows_all, features).astype(jnp.bfloat16)
        for h in range(halves):

            @pl.loop(0, span // COLUMNS)
            def _(j):
                here = pl.ds(pl.multiple_of(h * span + j * COLUMNS, 128), COLUMNS)
                result = jnp.dot(lhs[...], w[:, here], preferred_element_type=jnp.float32)
                result = result.reshape(n, part, COLUMNS)
                own[k, :, :, here] = result[:half]
                psend[k, :, :, here] = result[half:].astype(jnp.bfloat16)

            cols = pl.ds(h * span, span)
            core[k, h] = send(
                psend.at[k, :, :, cols],
                crecv.at[k, :, :, cols],
                csend_sem.at[k, h],
                crecv_sem.at[k, h],
                1,
            )

    order = [dz for dz in range(groups - 1, -1, -1) if dz % 2] + [
        dz for dz in range(groups - 1, -1, -1) if dz % 2 == 0
    ]

    def summed(k, s):
        return own[k, s] + crecv[k, s].astype(jnp.float32)

    def finish_core(k):
        for h in range(halves):
            core[k, h].wait_recv()
        for dz in order:
            ysend[k, dz] = summed(k, groups + groups - 1 - dz).astype(jnp.bfloat16)
            side[k, dz] = send(
                ysend.at[k, dz], yrecv.at[k, dz], ysend_sem.at[k, dz], yrecv_sem.at[k, dz], 2
            )

    def start_line(k, dz, bit, value):
        zsend[k, dz] = value.astype(jnp.bfloat16)
        line[k, dz] = send(
            zsend.at[k, dz], zrecv.at[k, dz], zsend_sem.at[k, dz], zrecv_sem.at[k, dz], 4 * bit
        )

    def finish_side(k):
        for dz in order:
            side[k, dz].wait_recv()
            value = summed(k, groups - 1 - dz) + yrecv[k, dz].astype(jnp.float32)
            if dz % 2:
                start_line(k, dz, 1, value)
            else:
                own[k, groups - 1 - dz] = value

    def finish_line(k, bit):
        for dz in range(groups - 2 * bit, -1, -2 * bit):
            line[k, dz + bit].wait_recv()
            value = own[k, groups - 1 - dz] + zrecv[k, dz + bit].astype(jnp.float32)
            if dz == 0 and 2 * bit == groups:
                out_ref[k] = value.astype(jnp.bfloat16)
            elif dz % (4 * bit):
                start_line(k, dz, 2 * bit, value)
            else:
                own[k, groups - 1 - dz] = value

    levels = groups.bit_length() - 1

    def settle(k, stage):
        if 0 <= k < chunks:
            if stage == 0:
                finish_side(k)
            else:
                finish_line(k, 1 << (stage - 1))

    for turn in range(chunks):
        multiply(turn)
        for stage in range(levels, -1, -1):
            settle(turn - LAG - stage, stage)
        finish_core(turn)
    done = chunks - 1 - LAG
    for turn in range(chunks, chunks + LAG + levels):
        for stage in range(levels, -1, -1):
            settle(turn - LAG - stage, stage)
    for copies in (dispatch, core, side, line):
        for copy in copies.values():
            copy.wait_send()


def scratch_of(n, tokens, chosen, features, width):
    chunks = tokens // PART
    groups, half = n // 4, n // 2
    small = jnp.bfloat16
    return [
        ((tokens, chosen, 2 * features), small),
        ((features, width), small),
        ((chunks, n, PART, features), small),
        ((chunks, n, PART, features), small),
        ((n * PART, features), small),
        ((chunks, half, PART, width), jnp.float32),
        ((chunks, half, PART, width), small),
        ((chunks, half, PART, width), small),
        ((chunks, groups, PART, width), small),
        ((chunks, groups, PART, width), small),
        ((chunks, groups, PART, width), small),
        ((chunks, groups, PART, width), small),
    ]


def bytes_of(buffers):
    total = 0
    for shape, kind in buffers:
        size = jnp.dtype(kind).itemsize
        for extent in shape:
            size *= extent
        total += size
    return total


def on_device(expert_ids, route_gates, routed_in, down_weight, slot_offset):
    n = lax.axis_size("ep")
    tokens, chosen = expert_ids.shape
    features, width = down_weight.shape[1:]
    buffers = scratch_of(n, tokens, chosen, features, width)
    if (
        n < 8
        or n & (n - 1)
        or tokens % PART
        or chosen % 8
        or features % TILE
        or width % (2 * COLUMNS)
        or bytes_of(buffers) > VMEM_LIMIT * 3 // 4
    ):
        return exchange_form(expert_ids, route_gates, routed_in, down_weight, slot_offset)
    chunks, groups = tokens // PART, n // 4
    dma = pltpu.SemaphoreType.DMA
    vmem = pl.BlockSpec(memory_space=pltpu.VMEM)
    result = pl.pallas_call(
        functools.partial(kernel, n),
        out_shape=jax.ShapeDtypeStruct((chunks, PART, width), jnp.bfloat16),
        in_specs=[pl.BlockSpec(memory_space=pltpu.SMEM), vmem, vmem]
        + [pl.BlockSpec(memory_space=pl.ANY)] * 2,
        out_specs=vmem,
        scratch_shapes=[pltpu.VMEM(shape, kind) for shape, kind in buffers]
        + [dma((1,)), dma((chunks,))]
        + [dma((chunks, n))] * 2
        + [dma((chunks, 2))] * 2
        + [dma((chunks, groups))] * 4,
        compiler_params=pltpu.CompilerParams(
            collective_id=0, has_side_effects=True, vmem_limit_bytes=VMEM_LIMIT
        ),
    )(slot_offset, expert_ids.T, route_gates.T, routed_in, down_weight)
    return result.reshape(tokens, width)


def solution(mesh):
    placed = (
        P(("grp", "ep"), None),
        P(("grp", "ep"), None),
        P(("grp", "ep"), None, None),
        P("ep", None, None),
        P(),
    )
    return jax.shard_map(
        on_device, mesh=mesh, in_specs=placed, out_specs=P(("grp", "ep"), None), check_vma=False
    )
```

```python
import functools

import jax
import jax.numpy as jnp
from jax import lax
from jax.experimental import pallas as pl
from jax.experimental.pallas import tpu as pltpu
from jax.sharding import PartitionSpec as P

MESH = pl.DeviceIdType.MESH
TILE = 256
COLUMNS = 896
PART = 8
LEAD = 2
AHEAD = 3
FINE = 2
FIRST, TURN = 8.0, 6.2
Y_FIRST, Y_TURN = 21.9, 6.2
Z_STEP, Z_FLOOR = (8.7, 8.0), 54.0
VMEM_LIMIT = 63 * 1024 * 1024


def swiglu(packed):
    half = packed.shape[-1] // 2
    gate = packed[..., :half].astype(jnp.float32)
    upper = packed[..., half:].astype(jnp.float32)
    return (jax.nn.silu(gate) * upper).astype(jnp.bfloat16)


def exchange_form(expert_ids, route_gates, routed_in, down_weight, slot_offset):
    experts = lax.axis_size("ep")
    tokens_here, chosen = expert_ids.shape
    pair_count = tokens_here * chosen
    capacity = 2 * pair_count // experts
    matrix = down_weight[0]
    offset = slot_offset[0]
    target = jnp.mod(expert_ids.reshape(pair_count) - offset, experts)
    onehot = (target[:, None] == jnp.arange(experts, dtype=jnp.int32)[None, :]).astype(jnp.int32)
    earlier = jnp.cumsum(onehot, axis=0) - onehot
    rank = jnp.sum(earlier * onehot, axis=1)
    row_index = target * capacity + rank
    source = (
        jnp.full((experts * capacity,), pair_count, jnp.int32)
        .at[row_index]
        .set(jnp.arange(pair_count, dtype=jnp.int32))
    )
    payload = swiglu(routed_in.reshape(pair_count, routed_in.shape[2]))
    padded = jnp.concatenate([payload, jnp.zeros((1, payload.shape[1]), jnp.bfloat16)], axis=0)
    outgoing = jnp.take(padded, source, axis=0).reshape(experts, capacity, payload.shape[1])
    results = jnp.einsum(
        "nkf,fd->nkd",
        lax.all_to_all(outgoing, "ep", split_axis=0, concat_axis=0, tiled=True),
        matrix,
        preferred_element_type=jnp.float32,
    ).astype(jnp.bfloat16)
    returned = lax.all_to_all(results, "ep", split_axis=0, concat_axis=0, tiled=True)
    width = returned.shape[2]
    picked = jnp.take(returned.reshape(experts * capacity, width), row_index, axis=0).reshape(
        tokens_here, chosen, width
    )
    total = jnp.zeros((tokens_here, width), jnp.float32)
    for choice_index in range(chosen):
        total = total + route_gates[:, choice_index, None] * picked[:, choice_index].astype(
            jnp.float32
        )
    return total.astype(jnp.bfloat16)


def flipped(index, distance):
    result, bit = index, 1
    while bit <= distance:
        if distance & bit:
            result = result + bit - 2 * bit * lax.rem(lax.div(index, bit), 2)
        bit *= 2
    return result


def slot_distance(n, slot):
    groups = n // 4
    return (groups - 1 - slot % groups) * 4 + (slot // groups % 2) * 2 + slot // (2 * groups)


def kernel(
    n,
    offset_ref,
    ids_ref,
    gate_ref,
    x_hbm,
    w_hbm,
    out_ref,
    x,
    w,
    outg,
    recv,
    lhs,
    own,
    psend,
    crecv,
    ysend,
    yrecv,
    zsend,
    zrecv,
    wsem,
    xsem,
    dsend_sem,
    drecv_sem,
    csend_sem,
    crecv_sem,
    ysend_sem,
    yrecv_sem,
    zsend_sem,
    zrecv_sem,
):
    me = lax.axis_index("ep")
    features, width = w.shape
    chunks, _, part, _ = recv.shape
    chosen = ids_ref.shape[0]
    pairs = part * chosen
    rows_all = n * part
    groups = n // 4
    half = n // 2
    line_at = me // 4
    at_end = jnp.logical_or(line_at == 0, line_at == groups - 1)

    def remote(src, dst, send_sem, recv_sem, distance):
        return pltpu.make_async_remote_copy(
            src_ref=src,
            dst_ref=dst,
            send_sem=send_sem,
            recv_sem=recv_sem,
            device_id={"ep": flipped(me, distance)},
            device_id_type=MESH,
        )

    def send(*args):
        copy = remote(*args)
        copy.start()
        return copy

    def fine(k):
        return k >= chunks - FINE

    barrier = pltpu.get_barrier_semaphore()
    for d in range(1, n):
        pl.semaphore_signal(barrier, inc=1, device_id={"ep": flipped(me, d)}, device_id_type=MESH)
    x_copies = []
    for k in range(chunks):
        tokens_of = pl.ds(k * part, part)
        x_copies.append(pltpu.make_async_copy(x_hbm.at[tokens_of], x.at[tokens_of], xsem.at[k]))
        x_copies[k].start()
    w_copy = pltpu.make_async_copy(w_hbm.at[0], w, wsem.at[0])
    w_copy.start()

    slots = [slot_distance(n, s) for s in range(n)]
    peers = [flipped(me, d) for d in slots]
    target_all = lax.rem(ids_ref[...] - offset_ref[0] + n, n).astype(jnp.float32).T
    gates_all = gate_ref[...].T
    lane = lax.broadcasted_iota(jnp.int32, (chosen, pairs), 1)
    spread = (lane % chosen == lax.broadcasted_iota(jnp.int32, (chosen, pairs), 0)).astype(jnp.bfloat16)
    mine = (
        lax.broadcasted_iota(jnp.int32, (rows_all, pairs), 1) // chosen
        == lax.broadcasted_iota(jnp.int32, (rows_all, pairs), 0) % part
    )
    peer_of = jnp.concatenate([jnp.full((part, chosen), e, jnp.int32) for e in peers], axis=0).astype(
        jnp.float32
    )

    dispatch = {}
    others = [s for s, d in enumerate(slots) if d]
    for k in range(chunks):
        for place, s in enumerate(others):
            dispatch[k, slots[s]] = remote(
                outg.at[k, place], recv.at[k, s], dsend_sem.at[0], drecv_sem.at[k], slots[s]
            )

    def issue(k, lines):
        if k < chunks:
            for dz in lines:
                for low in (2, 3, 0, 1):
                    if dz * 4 + low:
                        dispatch[k, dz * 4 + low].start()

    near, far = (0, 1), tuple(range(groups - 1, 1, -1))

    def issue_early(k):
        issue(k, (0,))

        @pl.when(jnp.logical_not(at_end))
        def _():
            issue(k, (1,) if k > AHEAD else far + (1,))

        @pl.when(at_end)
        def _():
            if k < LEAD + 2:
                issue(k, (1,))
            if 0 < k <= LEAD:
                issue(k - 1, far)

    def issue_late(k):
        @pl.when(jnp.logical_not(at_end))
        def _():
            if k + AHEAD + 1 < chunks:
                issue(k + AHEAD + 1, far)

        @pl.when(at_end)
        def _():
            issue(k + LEAD + 2, (1,))
            issue(k + LEAD, far)

    for k in range(chunks):
        target = target_all[k * part : (k + 1) * part]
        gates = gates_all[k * part : (k + 1) * part]
        hit = jnp.where(jnp.concatenate([target] * n, axis=0) == peer_of, 1.0, 0.0)
        scale = jnp.sum(hit * jnp.concatenate([gates] * n, axis=0), axis=1, keepdims=True)
        wanted = jnp.dot(hit.astype(jnp.bfloat16), spread, preferred_element_type=jnp.float32)
        pick = jnp.where(mine, wanted, 0.0).astype(jnp.bfloat16)
        x_copies[k].wait()
        for c in range(0, features, TILE):
            gate = x[k * part : (k + 1) * part, :, c : c + TILE].astype(jnp.float32)
            upper = x[k * part : (k + 1) * part, :, features + c : features + c + TILE].astype(jnp.float32)
            hidden = (jax.nn.silu(gate) * upper).reshape(pairs, TILE).astype(jnp.bfloat16)
            rows = jnp.dot(pick, hidden, preferred_element_type=jnp.float32)
            rows = (rows * scale).reshape(n, part, TILE).astype(jnp.bfloat16)
            for s, d in enumerate(slots):
                if d:
                    outg[k, others.index(s), :, c : c + TILE] = rows[s]
                else:
                    recv[k, s, :, c : c + TILE] = rows[s]
        if k == 0:
            pl.semaphore_wait(barrier, n - 1)
        issue_early(k)
    w_copy.wait()

    core, side, line = {}, {}, {}
    sums = [dz for dz in range(groups - 1, -1, -1) if dz % 2]
    sums += [dz for dz in range(groups - 1, -1, -1) if dz % 2 == 0]
    place_of = {dz: place for place, dz in enumerate(sums)}

    def multiply(k):
        remote(outg.at[k], recv.at[k, pl.ds(0, n - 1)], dsend_sem.at[0], drecv_sem.at[k], 1).wait_recv()
        issue_late(k)
        lhs[...] = recv[k].astype(jnp.float32).reshape(rows_all, features).astype(jnp.bfloat16)
        parts = 2 if fine(k) else 1
        span = width // parts
        for h in range(parts):

            @pl.loop(0, span // COLUMNS)
            def _(j):
                here = pl.ds(pl.multiple_of(h * span + j * COLUMNS, 128), COLUMNS)
                result = jnp.dot(lhs[...], w[:, here], preferred_element_type=jnp.float32)
                result = result.reshape(n, part, COLUMNS)
                own[k, :, :, here] = result[:half]
                psend[k, :, :, here] = result[half:].astype(jnp.bfloat16)

            cols = pl.ds(h * span, span)
            core[k, h] = send(
                psend.at[k, :, :, cols],
                crecv.at[k, :, :, cols],
                csend_sem.at[0],
                crecv_sem.at[k, h],
                1,
            )

    def summed(k, s):
        return own[k, s] + crecv[k, s].astype(jnp.float32)

    def pieces(k, members):
        return [[dz] for dz in members] if fine(k) else [members]

    def finish_core(k):
        for h in range(2 if fine(k) else 1):
            core[k, h].wait_recv()
        for piece in pieces(k, sums):
            for dz in piece:
                ysend[k, place_of[dz]] = summed(k, groups + groups - 1 - dz).astype(jnp.bfloat16)
            here = pl.ds(place_of[piece[0]], len(piece))
            side[k, piece[0]] = send(
                ysend.at[k, here], yrecv.at[k, here], ysend_sem.at[0], yrecv_sem.at[k, place_of[piece[0]]], 2
            )

    def start_line(k, bit):
        members = [dz for dz in sums if dz % (2 * bit) == bit]
        for piece in pieces(k, members):
            for dz in piece:
                if bit == 1:
                    if (k, dz) in side:
                        side[k, dz].wait_recv()
                    value = summed(k, groups - 1 - dz) + yrecv[k, place_of[dz]].astype(jnp.float32)
                else:
                    value = add_line(k, dz, bit // 2)
                zsend[k, place_of[dz]] = value.astype(jnp.bfloat16)
            here = pl.ds(place_of[piece[0]], len(piece))
            line[k, piece[0]] = send(
                zsend.at[k, here],
                zrecv.at[k, here],
                zsend_sem.at[0],
                zrecv_sem.at[k, place_of[piece[0]]],
                4 * bit,
            )

    def add_line(k, dz, bit):
        if (k, dz + bit) in line:
            line[k, dz + bit].wait_recv()
        return own[k, groups - 1 - dz] + zrecv[k, place_of[dz + bit]].astype(jnp.float32)

    def finish_side(k):
        start_line(k, 1)
        for dz in sums:
            if dz % 2 == 0:
                if (k, dz) in side:
                    side[k, dz].wait_recv()
                own[k, groups - 1 - dz] = summed(k, groups - 1 - dz) + yrecv[k, place_of[dz]].astype(
                    jnp.float32
                )

    def finish_line(k, bit):
        if 2 * bit < groups:
            start_line(k, 2 * bit)
        for dz in sums:
            if dz % (4 * bit) == 0:
                value = add_line(k, dz, bit)
                if 2 * bit == groups:
                    out_ref[k] = value.astype(jnp.bfloat16)
                else:
                    own[k, groups - 1 - dz] = value

    levels = groups.bit_length() - 1

    events = []
    for k in range(chunks):
        events.append((FIRST + TURN * k, k, multiply, ()))
        events.append((FIRST + TURN * k + 2.5, k, finish_core, ()))
        summed_at = Y_FIRST + Y_TURN * k
        events.append((summed_at, k, finish_side, ()))
        for level in range(levels):
            summed_at = max(summed_at + Z_STEP[min(level, 1)], Z_FLOOR * level)
            events.append((summed_at + 0.1 * k * level, k, finish_line, (1 << level,)))
    for _, k, step, rest in sorted(events, key=lambda event: event[:2]):
        step(k, *rest)
    for buffer, sem in ((outg, dsend_sem), (psend, csend_sem), (ysend, ysend_sem), (zsend, zsend_sem)):
        remote(buffer, buffer, sem.at[0], sem.at[0], 1).wait_send()


def scratch_of(n, tokens, chosen, features, width):
    chunks = tokens // PART
    groups, half = n // 4, n // 2
    small = jnp.bfloat16
    return [
        ((tokens, chosen, 2 * features), small),
        ((features, width), small),
        ((chunks, n - 1, PART, features), small),
        ((chunks, n, PART, features), small),
        ((n * PART, features), small),
        ((chunks, half, PART, width), jnp.float32),
        ((chunks, half, PART, width), small),
        ((chunks, half, PART, width), small),
        ((chunks, groups, PART, width), small),
        ((chunks, groups, PART, width), small),
        ((chunks, groups - 1, PART, width), small),
        ((chunks, groups - 1, PART, width), small),
    ]


def bytes_of(buffers):
    total = 0
    for shape, kind in buffers:
        size = jnp.dtype(kind).itemsize
        for extent in shape:
            size *= extent
        total += size
    return total


def on_device(expert_ids, route_gates, routed_in, down_weight, slot_offset):
    n = lax.axis_size("ep")
    tokens, chosen = expert_ids.shape
    features, width = down_weight.shape[1:]
    buffers = scratch_of(n, tokens, chosen, features, width)
    if (
        n < 8
        or n & (n - 1)
        or tokens % PART
        or chosen % 8
        or features % TILE
        or width % (2 * COLUMNS)
        or bytes_of(buffers) > VMEM_LIMIT * 3 // 4
    ):
        return exchange_form(expert_ids, route_gates, routed_in, down_weight, slot_offset)
    chunks, groups = tokens // PART, n // 4
    dma = pltpu.SemaphoreType.DMA
    vmem = pl.BlockSpec(memory_space=pltpu.VMEM)
    result = pl.pallas_call(
        functools.partial(kernel, n),
        out_shape=jax.ShapeDtypeStruct((chunks, PART, width), jnp.bfloat16),
        in_specs=[pl.BlockSpec(memory_space=pltpu.SMEM), vmem, vmem]
        + [pl.BlockSpec(memory_space=pl.ANY)] * 2,
        out_specs=vmem,
        scratch_shapes=[pltpu.VMEM(shape, kind) for shape, kind in buffers]
        + [dma((1,)), dma((chunks,))]
        + [dma((1,)), dma((chunks,))]
        + [dma((1,)), dma((chunks, 2))]
        + [dma((1,)), dma((chunks, groups))] * 2,
        compiler_params=pltpu.CompilerParams(
            collective_id=0, has_side_effects=True, vmem_limit_bytes=VMEM_LIMIT
        ),
    )(slot_offset, expert_ids.T, route_gates.T, routed_in, down_weight)
    return result.reshape(tokens, width)


def solution(mesh):
    placed = (
        P(("grp", "ep"), None),
        P(("grp", "ep"), None),
        P(("grp", "ep"), None, None),
        P("ep", None, None),
        P(),
    )
    return jax.shard_map(
        on_device, mesh=mesh, in_specs=placed, out_specs=P(("grp", "ep"), None), check_vma=False
    )
```

```python
import functools

import jax
import jax.numpy as jnp
from jax import lax
from jax.experimental import pallas as pl
from jax.experimental.pallas import tpu as pltpu
from jax.sharding import PartitionSpec as P

MESH = pl.DeviceIdType.MESH
TILE = 256
COLUMNS = 896
PART = 8
LEAD, AHEAD = 2, 3
FINE, DEFER = 2, 5
FIRST, TURN = 8.0, 6.2
Y_LAG, Z_LAG = 15.1, 6.5
EARLY, LATE = 54.2, 100.0
VMEM_LIMIT = 48 * 1024 * 1024


def swiglu(packed):
    half = packed.shape[-1] // 2
    gate = packed[..., :half].astype(jnp.float32)
    upper = packed[..., half:].astype(jnp.float32)
    return (jax.nn.silu(gate) * upper).astype(jnp.bfloat16)


def exchange_form(expert_ids, route_gates, routed_in, down_weight, slot_offset):
    experts = lax.axis_size("ep")
    tokens_here, chosen = expert_ids.shape
    pair_count = tokens_here * chosen
    capacity = 2 * pair_count // experts
    matrix = down_weight[0]
    offset = slot_offset[0]
    target = jnp.mod(expert_ids.reshape(pair_count) - offset, experts)
    onehot = (target[:, None] == jnp.arange(experts, dtype=jnp.int32)[None, :]).astype(jnp.int32)
    earlier = jnp.cumsum(onehot, axis=0) - onehot
    rank = jnp.sum(earlier * onehot, axis=1)
    row_index = target * capacity + rank
    source = (
        jnp.full((experts * capacity,), pair_count, jnp.int32)
        .at[row_index]
        .set(jnp.arange(pair_count, dtype=jnp.int32))
    )
    payload = swiglu(routed_in.reshape(pair_count, routed_in.shape[2]))
    padded = jnp.concatenate([payload, jnp.zeros((1, payload.shape[1]), jnp.bfloat16)], axis=0)
    outgoing = jnp.take(padded, source, axis=0).reshape(experts, capacity, payload.shape[1])
    results = jnp.einsum(
        "nkf,fd->nkd",
        lax.all_to_all(outgoing, "ep", split_axis=0, concat_axis=0, tiled=True),
        matrix,
        preferred_element_type=jnp.float32,
    ).astype(jnp.bfloat16)
    returned = lax.all_to_all(results, "ep", split_axis=0, concat_axis=0, tiled=True)
    width = returned.shape[2]
    picked = jnp.take(returned.reshape(experts * capacity, width), row_index, axis=0).reshape(
        tokens_here, chosen, width
    )
    total = jnp.zeros((tokens_here, width), jnp.float32)
    for choice_index in range(chosen):
        total = total + route_gates[:, choice_index, None] * picked[:, choice_index].astype(
            jnp.float32
        )
    return total.astype(jnp.bfloat16)


def flipped(index, distance):
    result, bit = index, 1
    while bit <= distance:
        if distance & bit:
            result = result + bit - 2 * bit * lax.rem(lax.div(index, bit), 2)
        bit *= 2
    return result


def slot_distance(n, slot):
    groups = n // 4
    return (groups - 1 - slot % groups) * 4 + (slot // groups % 2) * 2 + slot // (2 * groups)


def is_fine(k, chunks):
    return k >= chunks - FINE


def core_parts(k, chunks):
    return 2 if is_fine(k, chunks) else 1


def side_pieces(k, chunks, groups):
    sums = list(range(groups - 1, -1, -1))
    if is_fine(k, chunks):
        return [[dz] for dz in sums]
    return [sums[:-1], sums[-1:]] if k >= chunks - DEFER else [sums]


def semaphore_plan(chunks, groups):
    keys = ["w", "ids", "gates", "x_first", "x_rest", "dispatch_out", "core_out", "side_out", "line_out"]
    for k in range(chunks):
        keys.append(("dispatch", k))
        keys += [("core", k, h) for h in range(core_parts(k, chunks))]
        keys += [("side", k, piece[0]) for piece in side_pieces(k, chunks, groups)]
        keys += [("pair", k), ("next", k), ("last", k)]
    return {key: place for place, key in enumerate(keys)}


def kernel(
    n,
    offset_ref,
    ids_hbm,
    gate_hbm,
    x_hbm,
    w_hbm,
    out_ref,
    ids,
    gates,
    x,
    w,
    outg,
    recv,
    lhs,
    own,
    psend,
    crecv,
    ysend,
    yrecv,
    zsend,
    zrecv,
    zlast,
    sems,
    ready,
):
    me = lax.axis_index("ep")
    features, width = w.shape
    chunks, _, part, _ = recv.shape
    chosen = ids.shape[0]
    pairs = part * chosen
    rows_all = n * part
    groups = n // 4
    half = n // 2
    line_at = me // 4
    at_end = jnp.logical_or(line_at == 0, line_at == groups - 1)
    inside = jnp.logical_not(at_end)
    plan = semaphore_plan(chunks, groups)

    def sem(*key):
        return sems.at[plan[key if len(key) > 1 else key[0]]]

    def remote(src, dst, send_sem, recv_sem, distance):
        return pltpu.make_async_remote_copy(
            src_ref=src,
            dst_ref=dst,
            send_sem=send_sem,
            recv_sem=recv_sem,
            device_id={"ep": flipped(me, distance)},
            device_id_type=MESH,
        )

    def local(src, dst, key):
        copy = pltpu.make_async_copy(src, dst, sem(key))
        copy.start()
        return copy

    def tell(semaphore, distance):
        pl.semaphore_signal(
            semaphore, inc=1, device_id={"ep": flipped(me, distance)}, device_id_type=MESH
        )

    barrier = pltpu.get_barrier_semaphore()
    for d in range(1, 8):
        tell(barrier, d)

    @pl.when(inside)
    def _():
        for d in range(12, 16):
            tell(barrier, d)

    ids_copy = local(ids_hbm, ids, "ids")
    gates_copy = local(gate_hbm, gates, "gates")
    first, later = pl.ds(0, part), pl.ds(part, (chunks - 1) * part)
    x_first = local(x_hbm.at[first], x.at[first], "x_first")
    x_rest = local(x_hbm.at[later], x.at[later], "x_rest")
    w_copy = local(w_hbm.at[0], w, "w")

    slots = [slot_distance(n, s) for s in range(n)]
    others = [s for s, d in enumerate(slots) if d]
    peers = [flipped(me, d) for d in slots]
    lane = lax.broadcasted_iota(jnp.int32, (chosen, pairs), 1)
    spread = (lane % chosen == lax.broadcasted_iota(jnp.int32, (chosen, pairs), 0)).astype(jnp.bfloat16)
    mine = (
        lax.broadcasted_iota(jnp.int32, (rows_all, pairs), 1) // chosen
        == lax.broadcasted_iota(jnp.int32, (rows_all, pairs), 0) % part
    )
    peer_of = jnp.concatenate([jnp.full((part, chosen), e, jnp.int32) for e in peers], axis=0).astype(
        jnp.float32
    )

    dispatch = {}
    for k in range(chunks):
        for place, s in enumerate(others):
            dispatch[k, slots[s]] = remote(
                outg.at[k, place], recv.at[k, s], sem("dispatch_out"), sem("dispatch", k), slots[s]
            )

    def issue(k, lines):
        if k < chunks:
            for dz in lines:
                for low in (2, 3, 0, 1):
                    if dz * 4 + low:
                        dispatch[k, dz * 4 + low].start()

    far = tuple(range(groups - 1, 1, -1))

    def issue_early(k):
        issue(k, (0,))

        @pl.when(inside)
        def _():
            if k == 0:
                issue(0, (3, 1))
                tell(ready, 4)
                tell(ready, 12)
            elif k == 1:
                pl.semaphore_wait(ready, 1)
                tell(ready, 4)
                issue(0, (2,))
                issue(1, far + (1,))
            else:
                issue(k, (1,) if k > AHEAD else far + (1,))

        @pl.when(at_end)
        def _():
            if k == 1:
                pl.semaphore_wait(ready, 2)
            if 0 < k <= LEAD:
                issue(k - 1, far)
            if k < LEAD + 2:
                issue(k, (1,))

    def issue_late(k):
        @pl.when(inside)
        def _():
            if k + AHEAD + 1 < chunks:
                issue(k + AHEAD + 1, far)

        @pl.when(at_end)
        def _():
            issue(k + LEAD + 2, (1,))
            issue(k + LEAD, far)

    ids_copy.wait()
    gates_copy.wait()
    target_all = lax.rem(ids[...] - offset_ref[0] + n, n).astype(jnp.float32).T
    gates_all = gates[...].T

    def prepare(k):
        target = target_all[k * part : (k + 1) * part]
        weight = gates_all[k * part : (k + 1) * part]
        hit = jnp.where(jnp.concatenate([target] * n, axis=0) == peer_of, 1.0, 0.0)
        scale = jnp.sum(hit * jnp.concatenate([weight] * n, axis=0), axis=1, keepdims=True)
        wanted = jnp.dot(hit.astype(jnp.bfloat16), spread, preferred_element_type=jnp.float32)
        pick = jnp.where(mine, wanted, 0.0).astype(jnp.bfloat16)
        if k == 0:
            x_first.wait()
        if k == 1:
            x_rest.wait()
        for c in range(0, features, TILE):
            gate = x[k * part : (k + 1) * part, :, c : c + TILE].astype(jnp.float32)
            upper = x[k * part : (k + 1) * part, :, features + c : features + c + TILE].astype(jnp.float32)
            hidden = (jax.nn.silu(gate) * upper).reshape(pairs, TILE).astype(jnp.bfloat16)
            rows = jnp.dot(pick, hidden, preferred_element_type=jnp.float32)
            rows = (rows * scale).reshape(n, part, TILE).astype(jnp.bfloat16)
            for s, d in enumerate(slots):
                if d:
                    outg[k, others.index(s), :, c : c + TILE] = rows[s]
                else:
                    recv[k, s, :, c : c + TILE] = rows[s]

    for k in range(chunks):
        prepare(k)
        if k == 0:
            pl.semaphore_wait(barrier, jnp.where(at_end, 7, 11))
        issue_early(k)
    w_copy.wait()

    core, side = {}, {}

    def multiply(k):
        remote(
            outg.at[k], recv.at[k, pl.ds(0, n - 1)], sem("dispatch_out"), sem("dispatch", k), 1
        ).wait_recv()
        issue_late(k)
        lhs[...] = recv[k].astype(jnp.float32).reshape(rows_all, features).astype(jnp.bfloat16)
        parts = core_parts(k, chunks)
        span = width // parts
        for h in range(parts):

            @pl.loop(0, span // COLUMNS)
            def _(j):
                here = pl.ds(pl.multiple_of(h * span + j * COLUMNS, 128), COLUMNS)
                result = jnp.dot(lhs[...], w[:, here], preferred_element_type=jnp.float32)
                result = result.reshape(n, part, COLUMNS)
                own[k, :, :, here] = result[:half]
                psend[k, :, :, here] = result[half:].astype(jnp.bfloat16)

            cols = pl.ds(h * span, span)
            core[k, h] = remote(
                psend.at[k, :, :, cols], crecv.at[k, :, :, cols], sem("core_out"), sem("core", k, h), 1
            )
            core[k, h].start()

    def summed(k, s):
        return own[k, s] + crecv[k, s].astype(jnp.float32)

    def at_dz(dz):
        return groups - 1 - dz

    def send_side(k, piece):
        here = pl.ds(at_dz(piece[0]), len(piece))
        side[k, piece[0]] = remote(
            ysend.at[k, here], yrecv.at[k, here], sem("side_out"), sem("side", k, piece[0]), 2
        )
        side[k, piece[0]].start()

    def finish_core(k):
        for h in range(core_parts(k, chunks)):
            core[k, h].wait_recv()
        for piece in side_pieces(k, chunks, groups):
            for dz in piece:
                ysend[k, at_dz(dz)] = summed(k, groups + at_dz(dz)).astype(jnp.bfloat16)
            if piece != [0]:
                send_side(k, piece)

    def finish_core_later(k):
        if [0] in side_pieces(k, chunks, groups):
            send_side(k, [0])

    def need_side(k, members):
        for piece in side_pieces(k, chunks, groups):
            if (k, piece[0]) in side and set(piece) & set(members):
                side.pop((k, piece[0])).wait_recv()

    def value_of(k, dz):
        return summed(k, at_dz(dz)) + yrecv[k, at_dz(dz)].astype(jnp.float32)

    def line_copy(kind, k, here, landing, distance):
        return remote(zsend.at[k, here], landing, sem("line_out"), sem(kind, k), distance)

    two, one = pl.ds(0, 2), pl.ds(2, 1)

    def start_line(k):
        need_side(k, (3, 2))

        @pl.when(at_end)
        def _():
            for dz in (3, 2):
                zsend[k, at_dz(dz)] = value_of(k, dz).astype(jnp.bfloat16)
            line_copy("pair", k, two, zrecv.at[k, two], 4).start()

        need_side(k, (1,))
        zsend[k, at_dz(1)] = value_of(k, 1).astype(jnp.bfloat16)
        line_copy("next", k, one, zrecv.at[k, one], 4).start()

    def pass_line(k):
        @pl.when(inside)
        def _():
            line_copy("pair", k, two, zrecv.at[k, two], 4).wait_recv()
            for dz, distance in ((2, 8), (3, 12)):
                added = zrecv[k, at_dz(5 - dz)].astype(jnp.float32)
                zsend[k, at_dz(dz)] = (value_of(k, dz) + added).astype(jnp.bfloat16)
                line_copy("last", k, pl.ds(at_dz(dz), 1), zlast.at[pl.ds(k, 1)], distance).start()

    def finish(k):
        need_side(k, (0,))
        line_copy("next", k, one, zrecv.at[k, one], 4).wait_recv()
        value = value_of(k, 0) + zrecv[k, at_dz(1)].astype(jnp.float32)
        line_copy("last", k, one, zlast.at[pl.ds(k, 1)], 4).wait_recv()
        out_ref[k] = (value + zlast[k].astype(jnp.float32)).astype(jnp.bfloat16)

    events = []
    for k in range(chunks):
        at = FIRST + TURN * k
        events.append((at, k, multiply))
        events.append((at + 2.5, k, finish_core))
        events.append((FIRST + TURN * (chunks - 1) + 2.55, k, finish_core_later))
        events.append((at + Y_LAG, k, start_line))
        events.append((at + Y_LAG + Z_LAG, k, pass_line))
        events.append((EARLY if k < chunks - DEFER else LATE, k, finish))
    for _, k, step in sorted(events, key=lambda event: event[:2]):
        step(k)
    for buffer, key in (
        (outg, "dispatch_out"),
        (psend, "core_out"),
        (ysend, "side_out"),
        (zsend, "line_out"),
    ):
        remote(buffer, buffer, sem(key), sem(key), 1).wait_send()


def scratch_of(n, tokens, chosen, features, width):
    chunks = tokens // PART
    groups, half = n // 4, n // 2
    small = jnp.bfloat16
    return [
        ((chosen, tokens), jnp.int32),
        ((chosen, tokens), jnp.float32),
        ((tokens, chosen, 2 * features), small),
        ((features, width), small),
        ((chunks, n - 1, PART, features), small),
        ((chunks, n, PART, features), small),
        ((n * PART, features), small),
        ((chunks, half, PART, width), jnp.float32),
        ((chunks, half, PART, width), small),
        ((chunks, half, PART, width), small),
        ((chunks, groups, PART, width), small),
        ((chunks, groups, PART, width), small),
        ((chunks, groups - 1, PART, width), small),
        ((chunks, groups - 1, PART, width), small),
        ((chunks, PART, width), small),
    ]


def bytes_of(buffers):
    total = 0
    for shape, kind in buffers:
        size = jnp.dtype(kind).itemsize
        for extent in shape:
            size *= extent
        total += size
    return total


def on_device(expert_ids, route_gates, routed_in, down_weight, slot_offset):
    n = lax.axis_size("ep")
    tokens, chosen = expert_ids.shape
    features, width = down_weight.shape[1:]
    buffers = scratch_of(n, tokens, chosen, features, width)
    if (
        n != 16
        or tokens % PART
        or tokens < 4 * PART
        or chosen % 8
        or features % TILE
        or width % (2 * COLUMNS)
        or bytes_of(buffers) > VMEM_LIMIT * 7 // 8
    ):
        return exchange_form(expert_ids, route_gates, routed_in, down_weight, slot_offset)
    chunks, groups = tokens // PART, n // 4
    in_hbm = [
        pltpu.with_memory_space_constraint(array, pltpu.HBM)
        for array in (expert_ids.T, route_gates.T, routed_in, down_weight)
    ]
    result = pl.pallas_call(
        functools.partial(kernel, n),
        out_shape=jax.ShapeDtypeStruct((chunks, PART, width), jnp.bfloat16),
        in_specs=[pl.BlockSpec(memory_space=pltpu.SMEM)] + [pl.BlockSpec(memory_space=pltpu.HBM)] * 4,
        out_specs=pl.BlockSpec(memory_space=pltpu.VMEM),
        scratch_shapes=[pltpu.VMEM(shape, kind) for shape, kind in buffers]
        + [pltpu.SemaphoreType.DMA((len(semaphore_plan(chunks, groups)),)), pltpu.SemaphoreType.REGULAR],
        compiler_params=pltpu.CompilerParams(
            collective_id=0, has_side_effects=True, vmem_limit_bytes=VMEM_LIMIT
        ),
    )(slot_offset, *in_hbm)
    return result.reshape(tokens, width)


def solution(mesh):
    placed = (
        P(("grp", "ep"), None),
        P(("grp", "ep"), None),
        P(("grp", "ep"), None, None),
        P("ep", None, None),
        P(),
    )
    return jax.shard_map(
        on_device, mesh=mesh, in_specs=placed, out_specs=P(("grp", "ep"), None), check_vma=False
    )
```

```python
import functools

import jax
import jax.numpy as jnp
from jax import lax
from jax.experimental import pallas as pl
from jax.experimental.pallas import tpu as pltpu
from jax.sharding import PartitionSpec as P

MESH = pl.DeviceIdType.MESH
TILE = 256
COLUMNS = 896
PART = 8
LEAD, AHEAD = 3, 3
FINE, DEFER, HOLD = 2, 5, 4
FIRST, TURN = 8.0, 6.2
Y_LAG, Z_LAG = 15.1, 6.5
EARLY, LATE = 54.2, 100.0
VMEM_LIMIT = 48 * 1024 * 1024


def swiglu(packed):
    half = packed.shape[-1] // 2
    gate = packed[..., :half].astype(jnp.float32)
    upper = packed[..., half:].astype(jnp.float32)
    return (jax.nn.silu(gate) * upper).astype(jnp.bfloat16)


def exchange_form(expert_ids, route_gates, routed_in, down_weight, slot_offset):
    experts = lax.axis_size("ep")
    tokens_here, chosen = expert_ids.shape
    pair_count = tokens_here * chosen
    capacity = 2 * pair_count // experts
    matrix = down_weight[0]
    offset = slot_offset[0]
    target = jnp.mod(expert_ids.reshape(pair_count) - offset, experts)
    onehot = (target[:, None] == jnp.arange(experts, dtype=jnp.int32)[None, :]).astype(jnp.int32)
    earlier = jnp.cumsum(onehot, axis=0) - onehot
    rank = jnp.sum(earlier * onehot, axis=1)
    row_index = target * capacity + rank
    source = (
        jnp.full((experts * capacity,), pair_count, jnp.int32)
        .at[row_index]
        .set(jnp.arange(pair_count, dtype=jnp.int32))
    )
    payload = swiglu(routed_in.reshape(pair_count, routed_in.shape[2]))
    padded = jnp.concatenate([payload, jnp.zeros((1, payload.shape[1]), jnp.bfloat16)], axis=0)
    outgoing = jnp.take(padded, source, axis=0).reshape(experts, capacity, payload.shape[1])
    results = jnp.einsum(
        "nkf,fd->nkd",
        lax.all_to_all(outgoing, "ep", split_axis=0, concat_axis=0, tiled=True),
        matrix,
        preferred_element_type=jnp.float32,
    ).astype(jnp.bfloat16)
    returned = lax.all_to_all(results, "ep", split_axis=0, concat_axis=0, tiled=True)
    width = returned.shape[2]
    picked = jnp.take(returned.reshape(experts * capacity, width), row_index, axis=0).reshape(
        tokens_here, chosen, width
    )
    total = jnp.zeros((tokens_here, width), jnp.float32)
    for choice_index in range(chosen):
        total = total + route_gates[:, choice_index, None] * picked[:, choice_index].astype(
            jnp.float32
        )
    return total.astype(jnp.bfloat16)


def flipped(index, distance):
    result, bit = index, 1
    while bit <= distance:
        if distance & bit:
            result = result + bit - 2 * bit * lax.rem(lax.div(index, bit), 2)
        bit *= 2
    return result


def slot_distance(n, slot):
    groups = n // 4
    return (groups - 1 - slot % groups) * 4 + (slot // groups % 2) * 2 + slot // (2 * groups)


def is_fine(k, chunks):
    return k >= chunks - FINE


def core_parts(k, chunks):
    return 2 if is_fine(k, chunks) else 1


def side_pieces(k, chunks, groups):
    sums = list(range(groups - 1, -1, -1))
    if is_fine(k, chunks):
        return [[dz] for dz in sums]
    return [sums[:-1], sums[-1:]] if k >= chunks - DEFER else [sums]


def semaphore_plan(chunks, groups):
    keys = ["w", "ids", "gates", "x_first", "x_rest", "dispatch_out", "core_out", "side_out", "line_out"]
    for k in range(chunks):
        keys.append(("dispatch", k))
        keys += [("core", k, h) for h in range(core_parts(k, chunks))]
        keys += [("side", k, piece[0]) for piece in side_pieces(k, chunks, groups)]
        keys += [("pair", k), ("next", k), ("last", k)]
    return {key: place for place, key in enumerate(keys)}


def kernel(
    n,
    offset_ref,
    ids_hbm,
    gate_hbm,
    x_hbm,
    w_hbm,
    out_ref,
    ids,
    gates,
    x,
    w,
    outg,
    recv,
    lhs,
    own,
    psend,
    crecv,
    ysend,
    yrecv,
    zsend,
    zrecv,
    zlast,
    sems,
    ready,
):
    me = lax.axis_index("ep")
    features, width = w.shape
    chunks, _, part, _ = recv.shape
    chosen = ids.shape[0]
    pairs = part * chosen
    rows_all = n * part
    groups = n // 4
    half = n // 2
    line_at = me // 4
    at_end = jnp.logical_or(line_at == 0, line_at == groups - 1)
    inside = jnp.logical_not(at_end)
    plan = semaphore_plan(chunks, groups)

    def sem(*key):
        return sems.at[plan[key if len(key) > 1 else key[0]]]

    def remote(src, dst, send_sem, recv_sem, distance):
        return pltpu.make_async_remote_copy(
            src_ref=src,
            dst_ref=dst,
            send_sem=send_sem,
            recv_sem=recv_sem,
            device_id={"ep": flipped(me, distance)},
            device_id_type=MESH,
        )

    def local(src, dst, key):
        copy = pltpu.make_async_copy(src, dst, sem(key))
        copy.start()
        return copy

    def tell(semaphore, distance):
        pl.semaphore_signal(
            semaphore, inc=1, device_id={"ep": flipped(me, distance)}, device_id_type=MESH
        )

    barrier = pltpu.get_barrier_semaphore()
    for d in range(1, 8):
        tell(barrier, d)

    @pl.when(inside)
    def _():
        for d in range(12, 16):
            tell(barrier, d)

    ids_copy = local(ids_hbm, ids, "ids")
    gates_copy = local(gate_hbm, gates, "gates")
    first, later = pl.ds(0, part), pl.ds(part, (chunks - 1) * part)
    x_first = local(x_hbm.at[first], x.at[first], "x_first")
    x_rest = local(x_hbm.at[later], x.at[later], "x_rest")
    w_copy = local(w_hbm.at[0], w, "w")

    slots = [slot_distance(n, s) for s in range(n)]
    others = [s for s, d in enumerate(slots) if d]
    peers = [flipped(me, d) for d in slots]
    lane = lax.broadcasted_iota(jnp.int32, (chosen, pairs), 1)
    spread = (lane % chosen == lax.broadcasted_iota(jnp.int32, (chosen, pairs), 0)).astype(jnp.bfloat16)
    mine = (
        lax.broadcasted_iota(jnp.int32, (rows_all, pairs), 1) // chosen
        == lax.broadcasted_iota(jnp.int32, (rows_all, pairs), 0) % part
    )
    peer_of = jnp.concatenate([jnp.full((part, chosen), e, jnp.int32) for e in peers], axis=0).astype(
        jnp.float32
    )

    dispatch = {}
    for k in range(chunks):
        for place, s in enumerate(others):
            dispatch[k, slots[s]] = remote(
                outg.at[k, place], recv.at[k, s], sem("dispatch_out"), sem("dispatch", k), slots[s]
            )

    def issue(k, lines):
        if k < chunks:
            for dz in lines:
                for low in (2, 3, 0, 1):
                    if dz * 4 + low:
                        dispatch[k, dz * 4 + low].start()

    far = tuple(range(groups - 1, 1, -1))

    def issue_early(k):
        issue(k, (0,))

        @pl.when(inside)
        def _():
            if k == 0:
                issue(0, (3, 1))
                tell(ready, 4)
                tell(ready, 12)
            elif k == 1:
                pl.semaphore_wait(ready, 1)
                tell(ready, 4)
                issue(0, (2,))
                issue(1, far + (1,))
            else:
                issue(k, (1,) if k > AHEAD else far + (1,))

        @pl.when(at_end)
        def _():
            if k == 1:
                pl.semaphore_wait(ready, 2)
            if 0 < k <= LEAD:
                issue(k - 1, far)
            if k < LEAD + 2:
                issue(k, (1,))

    def issue_late(k):
        @pl.when(inside)
        def _():
            if k + AHEAD + 1 < chunks:
                issue(k + AHEAD + 1, far)

        @pl.when(at_end)
        def _():
            issue(k + LEAD + 2, (1,))
            issue(k + LEAD, far)

    ids_copy.wait()
    gates_copy.wait()
    target_all = lax.rem(ids[...] - offset_ref[0] + n, n).astype(jnp.float32).T
    gates_all = gates[...].T

    def prepare(k):
        target = target_all[k * part : (k + 1) * part]
        weight = gates_all[k * part : (k + 1) * part]
        hit = jnp.where(jnp.concatenate([target] * n, axis=0) == peer_of, 1.0, 0.0)
        scale = jnp.sum(hit * jnp.concatenate([weight] * n, axis=0), axis=1, keepdims=True)
        wanted = jnp.dot(hit.astype(jnp.bfloat16), spread, preferred_element_type=jnp.float32)
        pick = jnp.where(mine, wanted, 0.0).astype(jnp.bfloat16)
        if k == 0:
            x_first.wait()
        if k == 1:
            x_rest.wait()
        for c in range(0, features, TILE):
            gate = x[k * part : (k + 1) * part, :, c : c + TILE].astype(jnp.float32)
            upper = x[k * part : (k + 1) * part, :, features + c : features + c + TILE].astype(jnp.float32)
            hidden = (jax.nn.silu(gate) * upper).reshape(pairs, TILE).astype(jnp.bfloat16)
            rows = jnp.dot(pick, hidden, preferred_element_type=jnp.float32)
            rows = (rows * scale).reshape(n, part, TILE).astype(jnp.bfloat16)
            for s, d in enumerate(slots):
                if d:
                    outg[k, others.index(s), :, c : c + TILE] = rows[s]
                else:
                    recv[k, s, :, c : c + TILE] = rows[s]

    for k in range(chunks):
        prepare(k)
        if k == 0:
            pl.semaphore_wait(barrier, jnp.where(at_end, 7, 11))
        issue_early(k)
    w_copy.wait()

    core, side = {}, {}

    def multiply(k):
        remote(
            outg.at[k], recv.at[k, pl.ds(0, n - 1)], sem("dispatch_out"), sem("dispatch", k), 1
        ).wait_recv()
        issue_late(k)
        lhs[...] = recv[k].astype(jnp.float32).reshape(rows_all, features).astype(jnp.bfloat16)
        parts = core_parts(k, chunks)
        span = width // parts
        for h in range(parts):

            @pl.loop(0, span // COLUMNS)
            def _(j):
                here = pl.ds(pl.multiple_of(h * span + j * COLUMNS, 128), COLUMNS)
                result = jnp.dot(lhs[...], w[:, here], preferred_element_type=jnp.float32)
                result = result.reshape(n, part, COLUMNS)
                own[k, :, :, here] = result[:half]
                psend[k, :, :, here] = result[half:].astype(jnp.bfloat16)

            cols = pl.ds(h * span, span)
            core[k, h] = remote(
                psend.at[k, :, :, cols], crecv.at[k, :, :, cols], sem("core_out"), sem("core", k, h), 1
            )
            core[k, h].start()

    def summed(k, s):
        return own[k, s] + crecv[k, s].astype(jnp.float32)

    def at_dz(dz):
        return groups - 1 - dz

    def send_side(k, piece):
        here = pl.ds(at_dz(piece[0]), len(piece))
        side[k, piece[0]] = remote(
            ysend.at[k, here], yrecv.at[k, here], sem("side_out"), sem("side", k, piece[0]), 2
        )
        side[k, piece[0]].start()

    def finish_core(k):
        for h in range(core_parts(k, chunks)):
            core[k, h].wait_recv()
        for piece in side_pieces(k, chunks, groups):
            for dz in piece:
                ysend[k, at_dz(dz)] = summed(k, groups + at_dz(dz)).astype(jnp.bfloat16)
            if piece != [0]:
                send_side(k, piece)

    def finish_core_later(k):
        if [0] in side_pieces(k, chunks, groups):
            send_side(k, [0])

    def need_side(k, members):
        for piece in side_pieces(k, chunks, groups):
            if (k, piece[0]) in side and set(piece) & set(members):
                side.pop((k, piece[0])).wait_recv()

    def value_of(k, dz):
        return summed(k, at_dz(dz)) + yrecv[k, at_dz(dz)].astype(jnp.float32)

    def line_copy(kind, k, here, landing, distance):
        return remote(zsend.at[k, here], landing, sem("line_out"), sem(kind, k), distance)

    two, one = pl.ds(0, 2), pl.ds(2, 1)

    def start_line(k):
        need_side(k, (3, 2))

        @pl.when(at_end)
        def _():
            for dz in (3, 2):
                zsend[k, at_dz(dz)] = value_of(k, dz).astype(jnp.bfloat16)
            line_copy("pair", k, two, zrecv.at[k, two], 4).start()

        need_side(k, (1,))
        zsend[k, at_dz(1)] = value_of(k, 1).astype(jnp.bfloat16)

        @pl.when(jnp.logical_or(inside, k < chunks - HOLD))
        def _():
            line_copy("next", k, one, zrecv.at[k, one], 4).start()

    def send_held(k):
        @pl.when(at_end)
        def _():
            line_copy("next", k, one, zrecv.at[k, one], 4).start()

    def pass_line(k):
        @pl.when(inside)
        def _():
            line_copy("pair", k, two, zrecv.at[k, two], 4).wait_recv()
            for dz, distance in ((2, 8), (3, 12)):
                added = zrecv[k, at_dz(5 - dz)].astype(jnp.float32)
                zsend[k, at_dz(dz)] = (value_of(k, dz) + added).astype(jnp.bfloat16)
                line_copy("last", k, pl.ds(at_dz(dz), 1), zlast.at[pl.ds(k, 1)], distance).start()

    def finish(k):
        need_side(k, (0,))
        line_copy("next", k, one, zrecv.at[k, one], 4).wait_recv()
        value = value_of(k, 0) + zrecv[k, at_dz(1)].astype(jnp.float32)
        line_copy("last", k, one, zlast.at[pl.ds(k, 1)], 4).wait_recv()
        out_ref[k] = (value + zlast[k].astype(jnp.float32)).astype(jnp.bfloat16)

    events = []
    last_at = FIRST + TURN * (chunks - 1)
    for k in range(chunks):
        at = FIRST + TURN * k
        events.append((at, k, multiply))
        events.append((at + 2.5, k, finish_core))
        events.append((last_at + 2.55, k, finish_core_later))
        events.append((at + Y_LAG, k, start_line))
        if k >= chunks - HOLD:
            events.append((last_at + Y_LAG + 0.01, k, send_held))
        events.append((at + Y_LAG + Z_LAG, k, pass_line))
        events.append((EARLY if k < chunks - DEFER else LATE, k, finish))
    for _, k, step in sorted(events, key=lambda event: event[:2]):
        step(k)
    for buffer, key in (
        (outg, "dispatch_out"),
        (psend, "core_out"),
        (ysend, "side_out"),
        (zsend, "line_out"),
    ):
        remote(buffer, buffer, sem(key), sem(key), 1).wait_send()


def scratch_of(n, tokens, chosen, features, width):
    chunks = tokens // PART
    groups, half = n // 4, n // 2
    small = jnp.bfloat16
    return [
        ((chosen, tokens), jnp.int32),
        ((chosen, tokens), jnp.float32),
        ((tokens, chosen, 2 * features), small),
        ((features, width), small),
        ((chunks, n - 1, PART, features), small),
        ((chunks, n, PART, features), small),
        ((n * PART, features), small),
        ((chunks, half, PART, width), jnp.float32),
        ((chunks, half, PART, width), small),
        ((chunks, half, PART, width), small),
        ((chunks, groups, PART, width), small),
        ((chunks, groups, PART, width), small),
        ((chunks, groups - 1, PART, width), small),
        ((chunks, groups - 1, PART, width), small),
        ((chunks, PART, width), small),
    ]


def bytes_of(buffers):
    total = 0
    for shape, kind in buffers:
        size = jnp.dtype(kind).itemsize
        for extent in shape:
            size *= extent
        total += size
    return total


def on_device(expert_ids, route_gates, routed_in, down_weight, slot_offset):
    n = lax.axis_size("ep")
    tokens, chosen = expert_ids.shape
    features, width = down_weight.shape[1:]
    buffers = scratch_of(n, tokens, chosen, features, width)
    if (
        n != 16
        or tokens % PART
        or tokens < 4 * PART
        or chosen % 8
        or features % TILE
        or width % (2 * COLUMNS)
        or bytes_of(buffers) > VMEM_LIMIT * 7 // 8
    ):
        return exchange_form(expert_ids, route_gates, routed_in, down_weight, slot_offset)
    chunks, groups = tokens // PART, n // 4
    in_hbm = [
        pltpu.with_memory_space_constraint(array, pltpu.HBM)
        for array in (expert_ids.T, route_gates.T, routed_in, down_weight)
    ]
    result = pl.pallas_call(
        functools.partial(kernel, n),
        out_shape=jax.ShapeDtypeStruct((chunks, PART, width), jnp.bfloat16),
        in_specs=[pl.BlockSpec(memory_space=pltpu.SMEM)] + [pl.BlockSpec(memory_space=pltpu.HBM)] * 4,
        out_specs=pl.BlockSpec(memory_space=pltpu.VMEM),
        scratch_shapes=[pltpu.VMEM(shape, kind) for shape, kind in buffers]
        + [pltpu.SemaphoreType.DMA((len(semaphore_plan(chunks, groups)),)), pltpu.SemaphoreType.REGULAR],
        compiler_params=pltpu.CompilerParams(
            collective_id=0, has_side_effects=True, vmem_limit_bytes=VMEM_LIMIT
        ),
    )(slot_offset, *in_hbm)
    return result.reshape(tokens, width)


def solution(mesh):
    placed = (
        P(("grp", "ep"), None),
        P(("grp", "ep"), None),
        P(("grp", "ep"), None, None),
        P("ep", None, None),
        P(),
    )
    return jax.shard_map(
        on_device, mesh=mesh, in_specs=placed, out_specs=P(("grp", "ep"), None), check_vma=False
    )
```

```python
import functools

import jax
import jax.numpy as jnp
from jax import lax
from jax.experimental import pallas as pl
from jax.experimental.pallas import tpu as pltpu
from jax.sharding import PartitionSpec as P

MESH = pl.DeviceIdType.MESH
TILE = 256
COLUMNS = 896
PART = 8
LEAD, AHEAD = 3, 3
FINE, DEFER, HOLD = 2, 5, 4
FIRST, TURN = 8.0, 6.2
Y_LAG, Z_LAG = 15.1, 6.5
EARLY, LATE = 54.2, 100.0
VMEM_LIMIT = 48 * 1024 * 1024


def swiglu(packed):
    half = packed.shape[-1] // 2
    gate = packed[..., :half].astype(jnp.float32)
    upper = packed[..., half:].astype(jnp.float32)
    return (jax.nn.silu(gate) * upper).astype(jnp.bfloat16)


def exchange_form(expert_ids, route_gates, routed_in, down_weight, slot_offset):
    experts = lax.axis_size("ep")
    tokens_here, chosen = expert_ids.shape
    pair_count = tokens_here * chosen
    capacity = 2 * pair_count // experts
    matrix = down_weight[0]
    offset = slot_offset[0]
    target = jnp.mod(expert_ids.reshape(pair_count) - offset, experts)
    onehot = (target[:, None] == jnp.arange(experts, dtype=jnp.int32)[None, :]).astype(jnp.int32)
    earlier = jnp.cumsum(onehot, axis=0) - onehot
    rank = jnp.sum(earlier * onehot, axis=1)
    row_index = target * capacity + rank
    source = (
        jnp.full((experts * capacity,), pair_count, jnp.int32)
        .at[row_index]
        .set(jnp.arange(pair_count, dtype=jnp.int32))
    )
    payload = swiglu(routed_in.reshape(pair_count, routed_in.shape[2]))
    padded = jnp.concatenate([payload, jnp.zeros((1, payload.shape[1]), jnp.bfloat16)], axis=0)
    outgoing = jnp.take(padded, source, axis=0).reshape(experts, capacity, payload.shape[1])
    results = jnp.einsum(
        "nkf,fd->nkd",
        lax.all_to_all(outgoing, "ep", split_axis=0, concat_axis=0, tiled=True),
        matrix,
        preferred_element_type=jnp.float32,
    ).astype(jnp.bfloat16)
    returned = lax.all_to_all(results, "ep", split_axis=0, concat_axis=0, tiled=True)
    width = returned.shape[2]
    picked = jnp.take(returned.reshape(experts * capacity, width), row_index, axis=0).reshape(
        tokens_here, chosen, width
    )
    total = jnp.zeros((tokens_here, width), jnp.float32)
    for choice_index in range(chosen):
        total = total + route_gates[:, choice_index, None] * picked[:, choice_index].astype(
            jnp.float32
        )
    return total.astype(jnp.bfloat16)


def flipped(index, distance):
    result, bit = index, 1
    while bit <= distance:
        if distance & bit:
            result = result + bit - 2 * bit * lax.rem(lax.div(index, bit), 2)
        bit *= 2
    return result


def slot_distance(n, slot):
    groups = n // 4
    return (groups - 1 - slot % groups) * 4 + (slot // groups % 2) * 2 + slot // (2 * groups)


def is_fine(k, chunks):
    return k >= chunks - FINE


def core_parts(k, chunks):
    return 2 if is_fine(k, chunks) else 1


def side_pieces(k, chunks, groups):
    sums = list(range(groups - 1, -1, -1))
    if is_fine(k, chunks):
        return [[dz] for dz in sums]
    return [sums[:-1], sums[-1:]] if k >= chunks - DEFER else [sums]


def pair_pieces(k, chunks):
    return [[3], [2]] if is_fine(k, chunks) else [[3, 2]]


def semaphore_plan(chunks, groups):
    keys = ["w", "ids", "gates", "x_first", "x_rest", "dispatch_out", "core_out", "side_out", "line_out"]
    for k in range(chunks):
        keys.append(("dispatch", k))
        keys += [("core", k, h) for h in range(core_parts(k, chunks))]
        keys += [("side", k, piece[0]) for piece in side_pieces(k, chunks, groups)]
        keys += [("pair", k, piece[0]) for piece in pair_pieces(k, chunks)]
        keys += [("next", k), ("last", k)]
    return {key: place for place, key in enumerate(keys)}


def kernel(
    n,
    offset_ref,
    ids_hbm,
    gate_hbm,
    x_hbm,
    w_hbm,
    out_ref,
    ids,
    gates,
    x,
    w,
    outg,
    recv,
    lhs,
    own,
    psend,
    crecv,
    ysend,
    yrecv,
    zsend,
    zrecv,
    zlast,
    sems,
    side_ready,
    ready,
):
    me = lax.axis_index("ep")
    features, width = w.shape
    chunks, _, part, _ = recv.shape
    chosen = ids.shape[0]
    pairs = part * chosen
    rows_all = n * part
    groups = n // 4
    half = n // 2
    line_at = me // 4
    at_end = jnp.logical_or(line_at == 0, line_at == groups - 1)
    inside = jnp.logical_not(at_end)
    plan = semaphore_plan(chunks, groups)

    def sem(*key):
        return sems.at[plan[key if len(key) > 1 else key[0]]]

    def remote(src, dst, send_sem, recv_sem, distance):
        return pltpu.make_async_remote_copy(
            src_ref=src,
            dst_ref=dst,
            send_sem=send_sem,
            recv_sem=recv_sem,
            device_id={"ep": flipped(me, distance)},
            device_id_type=MESH,
        )

    def local(src, dst, key):
        copy = pltpu.make_async_copy(src, dst, sem(key))
        copy.start()
        return copy

    def tell(semaphore, distance):
        pl.semaphore_signal(
            semaphore, inc=1, device_id={"ep": flipped(me, distance)}, device_id_type=MESH
        )

    barrier = pltpu.get_barrier_semaphore()
    for d in range(1, 6):
        tell(barrier, d)

    @pl.when(inside)
    def _():
        for d in (6, 7, 12, 13):
            tell(barrier, d)

    ids_copy = local(ids_hbm, ids, "ids")
    gates_copy = local(gate_hbm, gates, "gates")
    first, later = pl.ds(0, part), pl.ds(part, (chunks - 1) * part)
    x_first = local(x_hbm.at[first], x.at[first], "x_first")
    x_rest = local(x_hbm.at[later], x.at[later], "x_rest")
    w_copy = local(w_hbm.at[0], w, "w")

    slots = [slot_distance(n, s) for s in range(n)]
    others = [s for s, d in enumerate(slots) if d]
    peers = [flipped(me, d) for d in slots]
    lane = lax.broadcasted_iota(jnp.int32, (chosen, pairs), 1)
    spread = (lane % chosen == lax.broadcasted_iota(jnp.int32, (chosen, pairs), 0)).astype(jnp.bfloat16)
    mine = (
        lax.broadcasted_iota(jnp.int32, (rows_all, pairs), 1) // chosen
        == lax.broadcasted_iota(jnp.int32, (rows_all, pairs), 0) % part
    )
    peer_of = jnp.concatenate([jnp.full((part, chosen), e, jnp.int32) for e in peers], axis=0).astype(
        jnp.float32
    )

    dispatch = {}
    for k in range(chunks):
        for place, s in enumerate(others):
            dispatch[k, slots[s]] = remote(
                outg.at[k, place], recv.at[k, s], sem("dispatch_out"), sem("dispatch", k), slots[s]
            )

    straight, turning = (0, 1), (2, 3)

    def issue(k, lines, lows=turning + straight):
        if k < chunks:
            for dz in lines:
                for low in lows:
                    if dz * 4 + low:
                        dispatch[k, dz * 4 + low].start()

    far = tuple(range(groups - 1, 1, -1))

    def issue_early(k):
        issue(k, (0,))

        @pl.when(inside)
        def _():
            if k == 0:
                tell(side_ready, 2)
                issue(0, (3, 1), straight)
            elif k == 1:
                issue(1, (3,), straight)
                pl.semaphore_wait(side_ready, 1)
                tell(ready, 4)
                tell(ready, 12)
                issue(0, (3, 1), turning)
                pl.semaphore_wait(ready, 1)
                tell(ready, 4)
                issue(0, (2,))
                issue(1, (3,), turning)
                issue(1, (2, 1))
            else:
                issue(k, (1,) if k > AHEAD else far + (1,))

        @pl.when(at_end)
        def _():
            if k == 1:
                pl.semaphore_wait(ready, 2)
            if 0 < k <= LEAD:
                issue(k - 1, far)
            if k < LEAD + 2:
                issue(k, (1,))

    def issue_late(k):
        @pl.when(inside)
        def _():
            if k + AHEAD + 1 < chunks:
                issue(k + AHEAD + 1, far)

        @pl.when(at_end)
        def _():
            issue(k + LEAD + 2, (1,))
            issue(k + LEAD, far)

    ids_copy.wait()
    gates_copy.wait()
    target_all = lax.rem(ids[...] - offset_ref[0] + n, n).astype(jnp.float32).T
    gates_all = gates[...].T

    def prepare(k):
        target = target_all[k * part : (k + 1) * part]
        weight = gates_all[k * part : (k + 1) * part]
        hit = jnp.where(jnp.concatenate([target] * n, axis=0) == peer_of, 1.0, 0.0)
        scale = jnp.sum(hit * jnp.concatenate([weight] * n, axis=0), axis=1, keepdims=True)
        wanted = jnp.dot(hit.astype(jnp.bfloat16), spread, preferred_element_type=jnp.float32)
        pick = jnp.where(mine, wanted, 0.0).astype(jnp.bfloat16)
        if k == 0:
            x_first.wait()
        if k == 1:
            x_rest.wait()
        for c in range(0, features, TILE):
            gate = x[k * part : (k + 1) * part, :, c : c + TILE].astype(jnp.float32)
            upper = x[k * part : (k + 1) * part, :, features + c : features + c + TILE].astype(jnp.float32)
            hidden = (jax.nn.silu(gate) * upper).reshape(pairs, TILE).astype(jnp.bfloat16)
            rows = jnp.dot(pick, hidden, preferred_element_type=jnp.float32)
            rows = (rows * scale).reshape(n, part, TILE).astype(jnp.bfloat16)
            for s, d in enumerate(slots):
                if d:
                    outg[k, others.index(s), :, c : c + TILE] = rows[s]
                else:
                    recv[k, s, :, c : c + TILE] = rows[s]

    for k in range(chunks):
        prepare(k)
        if k == 0:
            pl.semaphore_wait(barrier, 7)
        issue_early(k)
    w_copy.wait()

    core, side = {}, {}

    def multiply(k):
        remote(
            outg.at[k], recv.at[k, pl.ds(0, n - 1)], sem("dispatch_out"), sem("dispatch", k), 1
        ).wait_recv()
        issue_late(k)
        lhs[...] = recv[k].astype(jnp.float32).reshape(rows_all, features).astype(jnp.bfloat16)
        parts = core_parts(k, chunks)
        span = width // parts
        for h in range(parts):

            @pl.loop(0, span // COLUMNS)
            def _(j):
                here = pl.ds(pl.multiple_of(h * span + j * COLUMNS, 128), COLUMNS)
                result = jnp.dot(lhs[...], w[:, here], preferred_element_type=jnp.float32)
                result = result.reshape(n, part, COLUMNS)
                own[k, :, :, here] = result[:half]
                psend[k, :, :, here] = result[half:].astype(jnp.bfloat16)

            cols = pl.ds(h * span, span)
            core[k, h] = remote(
                psend.at[k, :, :, cols], crecv.at[k, :, :, cols], sem("core_out"), sem("core", k, h), 1
            )
            core[k, h].start()

    def summed(k, s):
        return own[k, s] + crecv[k, s].astype(jnp.float32)

    def at_dz(dz):
        return groups - 1 - dz

    def send_side(k, piece):
        here = pl.ds(at_dz(piece[0]), len(piece))
        side[k, piece[0]] = remote(
            ysend.at[k, here], yrecv.at[k, here], sem("side_out"), sem("side", k, piece[0]), 2
        )
        side[k, piece[0]].start()

    def finish_core(k):
        for h in range(core_parts(k, chunks)):
            core[k, h].wait_recv()
        for piece in side_pieces(k, chunks, groups):
            for dz in piece:
                ysend[k, at_dz(dz)] = summed(k, groups + at_dz(dz)).astype(jnp.bfloat16)
            if piece != [0]:
                send_side(k, piece)

    def finish_core_later(k):
        if [0] in side_pieces(k, chunks, groups):
            send_side(k, [0])

    def need_side(k, members):
        for piece in side_pieces(k, chunks, groups):
            if (k, piece[0]) in side and set(piece) & set(members):
                side.pop((k, piece[0])).wait_recv()

    def value_of(k, dz):
        return summed(k, at_dz(dz)) + yrecv[k, at_dz(dz)].astype(jnp.float32)

    def line_copy(kind, k, here, landing, distance):
        return remote(zsend.at[k, here], landing, sem("line_out"), sem(kind, k), distance)

    def pair_copy(k, piece):
        here = pl.ds(at_dz(piece[0]), len(piece))
        return remote(zsend.at[k, here], zrecv.at[k, here], sem("line_out"), sem("pair", k, piece[0]), 4)

    one = pl.ds(2, 1)

    def start_line(k):
        for piece in pair_pieces(k, chunks):
            need_side(k, piece)

            @pl.when(at_end)
            def _():
                for dz in piece:
                    zsend[k, at_dz(dz)] = value_of(k, dz).astype(jnp.bfloat16)
                pair_copy(k, piece).start()

        need_side(k, (1,))
        zsend[k, at_dz(1)] = value_of(k, 1).astype(jnp.bfloat16)

        @pl.when(jnp.logical_or(inside, k < chunks - HOLD))
        def _():
            line_copy("next", k, one, zrecv.at[k, one], 4).start()

    def send_held(k):
        @pl.when(at_end)
        def _():
            line_copy("next", k, one, zrecv.at[k, one], 4).start()

    def pass_line(k):
        @pl.when(inside)
        def _():
            for piece in pair_pieces(k, chunks):
                pair_copy(k, piece).wait_recv()
                for landed in piece:
                    dz = 5 - landed
                    added = zrecv[k, at_dz(landed)].astype(jnp.float32)
                    zsend[k, at_dz(dz)] = (value_of(k, dz) + added).astype(jnp.bfloat16)
                    here = pl.ds(at_dz(dz), 1)
                    line_copy("last", k, here, zlast.at[pl.ds(k, 1)], 4 * dz).start()

    def finish(k):
        need_side(k, (0,))
        line_copy("next", k, one, zrecv.at[k, one], 4).wait_recv()
        value = value_of(k, 0) + zrecv[k, at_dz(1)].astype(jnp.float32)
        line_copy("last", k, one, zlast.at[pl.ds(k, 1)], 4).wait_recv()
        out_ref[k] = (value + zlast[k].astype(jnp.float32)).astype(jnp.bfloat16)

    events = []
    last_at = FIRST + TURN * (chunks - 1)
    for k in range(chunks):
        at = FIRST + TURN * k
        events.append((at, k, multiply))
        events.append((at + 2.5, k, finish_core))
        events.append((last_at + 2.55, k, finish_core_later))
        events.append((at + Y_LAG, k, start_line))
        if k >= chunks - HOLD:
            events.append((last_at + Y_LAG + 0.01, k, send_held))
        events.append((at + Y_LAG + Z_LAG, k, pass_line))
        events.append((EARLY if k < chunks - DEFER else LATE, k, finish))
    for _, k, step in sorted(events, key=lambda event: event[:2]):
        step(k)
    for buffer, key in (
        (outg, "dispatch_out"),
        (psend, "core_out"),
        (ysend, "side_out"),
        (zsend, "line_out"),
    ):
        remote(buffer, buffer, sem(key), sem(key), 1).wait_send()


def scratch_of(n, tokens, chosen, features, width):
    chunks = tokens // PART
    groups, half = n // 4, n // 2
    small = jnp.bfloat16
    return [
        ((chosen, tokens), jnp.int32),
        ((chosen, tokens), jnp.float32),
        ((tokens, chosen, 2 * features), small),
        ((features, width), small),
        ((chunks, n - 1, PART, features), small),
        ((chunks, n, PART, features), small),
        ((n * PART, features), small),
        ((chunks, half, PART, width), jnp.float32),
        ((chunks, half, PART, width), small),
        ((chunks, half, PART, width), small),
        ((chunks, groups, PART, width), small),
        ((chunks, groups, PART, width), small),
        ((chunks, groups - 1, PART, width), small),
        ((chunks, groups - 1, PART, width), small),
        ((chunks, PART, width), small),
    ]


def bytes_of(buffers):
    total = 0
    for shape, kind in buffers:
        size = jnp.dtype(kind).itemsize
        for extent in shape:
            size *= extent
        total += size
    return total


def on_device(expert_ids, route_gates, routed_in, down_weight, slot_offset):
    n = lax.axis_size("ep")
    tokens, chosen = expert_ids.shape
    features, width = down_weight.shape[1:]
    buffers = scratch_of(n, tokens, chosen, features, width)
    if (
        n != 16
        or tokens % PART
        or tokens < 4 * PART
        or chosen % 8
        or features % TILE
        or width % (2 * COLUMNS)
        or bytes_of(buffers) > VMEM_LIMIT * 7 // 8
    ):
        return exchange_form(expert_ids, route_gates, routed_in, down_weight, slot_offset)
    chunks, groups = tokens // PART, n // 4
    in_hbm = [
        pltpu.with_memory_space_constraint(array, pltpu.HBM)
        for array in (expert_ids.T, route_gates.T, routed_in, down_weight)
    ]
    result = pl.pallas_call(
        functools.partial(kernel, n),
        out_shape=jax.ShapeDtypeStruct((chunks, PART, width), jnp.bfloat16),
        in_specs=[pl.BlockSpec(memory_space=pltpu.SMEM)] + [pl.BlockSpec(memory_space=pltpu.HBM)] * 4,
        out_specs=pl.BlockSpec(memory_space=pltpu.VMEM),
        scratch_shapes=[pltpu.VMEM(shape, kind) for shape, kind in buffers]
        + [pltpu.SemaphoreType.DMA((len(semaphore_plan(chunks, groups)),)), pltpu.SemaphoreType.REGULAR, pltpu.SemaphoreType.REGULAR],
        compiler_params=pltpu.CompilerParams(
            collective_id=0, has_side_effects=True, vmem_limit_bytes=VMEM_LIMIT
        ),
    )(slot_offset, *in_hbm)
    return result.reshape(tokens, width)


def solution(mesh):
    placed = (
        P(("grp", "ep"), None),
        P(("grp", "ep"), None),
        P(("grp", "ep"), None, None),
        P("ep", None, None),
        P(),
    )
    return jax.shard_map(
        on_device, mesh=mesh, in_specs=placed, out_specs=P(("grp", "ep"), None), check_vma=False
    )
```

```python
import functools

import jax
import jax.numpy as jnp
from jax import lax
from jax.experimental import pallas as pl
from jax.experimental.pallas import tpu as pltpu
from jax.sharding import PartitionSpec as P

MESH = pl.DeviceIdType.MESH
TILE = 256
COLUMNS = 1792
PART = 8
LEAD, AHEAD = 3, 3
FINE, DEFER, HOLD = 2, 5, 4
FIRST, TURN = 8.0, 6.2
Y_LAG, Z_LAG = 15.1, 6.5
SKIP = 2
EARLY, LATE = 54.2, 100.0
VMEM_LIMIT = 48 * 1024 * 1024


def swiglu(packed):
    half = packed.shape[-1] // 2
    gate = packed[..., :half].astype(jnp.float32)
    upper = packed[..., half:].astype(jnp.float32)
    return (jax.nn.silu(gate) * upper).astype(jnp.bfloat16)


def exchange_form(expert_ids, route_gates, routed_in, down_weight, slot_offset):
    experts = lax.axis_size("ep")
    tokens_here, chosen = expert_ids.shape
    pair_count = tokens_here * chosen
    capacity = 2 * pair_count // experts
    matrix = down_weight[0]
    offset = slot_offset[0]
    target = jnp.mod(expert_ids.reshape(pair_count) - offset, experts)
    onehot = (target[:, None] == jnp.arange(experts, dtype=jnp.int32)[None, :]).astype(jnp.int32)
    earlier = jnp.cumsum(onehot, axis=0) - onehot
    rank = jnp.sum(earlier * onehot, axis=1)
    row_index = target * capacity + rank
    source = (
        jnp.full((experts * capacity,), pair_count, jnp.int32)
        .at[row_index]
        .set(jnp.arange(pair_count, dtype=jnp.int32))
    )
    payload = swiglu(routed_in.reshape(pair_count, routed_in.shape[2]))
    padded = jnp.concatenate([payload, jnp.zeros((1, payload.shape[1]), jnp.bfloat16)], axis=0)
    outgoing = jnp.take(padded, source, axis=0).reshape(experts, capacity, payload.shape[1])
    results = jnp.einsum(
        "nkf,fd->nkd",
        lax.all_to_all(outgoing, "ep", split_axis=0, concat_axis=0, tiled=True),
        matrix,
        preferred_element_type=jnp.float32,
    ).astype(jnp.bfloat16)
    returned = lax.all_to_all(results, "ep", split_axis=0, concat_axis=0, tiled=True)
    width = returned.shape[2]
    picked = jnp.take(returned.reshape(experts * capacity, width), row_index, axis=0).reshape(
        tokens_here, chosen, width
    )
    total = jnp.zeros((tokens_here, width), jnp.float32)
    for choice_index in range(chosen):
        total = total + route_gates[:, choice_index, None] * picked[:, choice_index].astype(
            jnp.float32
        )
    return total.astype(jnp.bfloat16)


def flipped(index, distance):
    result, bit = index, 1
    while bit <= distance:
        if distance & bit:
            result = result + bit - 2 * bit * lax.rem(lax.div(index, bit), 2)
        bit *= 2
    return result


def slot_distance(n, slot):
    groups = n // 4
    return (groups - 1 - slot % groups) * 4 + (slot // groups % 2) * 2 + slot // (2 * groups)


def is_fine(k, chunks):
    return k >= chunks - FINE


def core_parts(k, chunks):
    return 2 if is_fine(k, chunks) else 1


def side_pieces(k, chunks, groups):
    sums = list(range(groups - 1, -1, -1))
    if is_fine(k, chunks):
        return [[dz] for dz in sums]
    return [sums[:-1], sums[-1:]] if k >= chunks - DEFER else [sums]


def pair_pieces(k, chunks):
    return [[3], [2]] if is_fine(k, chunks) else [[3, 2]]


def semaphore_plan(chunks, groups):
    keys = ["w", "ids", "gates", "x_first", "x_rest", "dispatch_out", "core_out", "side_out", "line_out"]
    for k in range(chunks):
        keys.append(("dispatch", k))
        keys += [("core", k, h) for h in range(core_parts(k, chunks))]
        keys += [("side", k, piece[0]) for piece in side_pieces(k, chunks, groups)]
        keys += [("pair", k, piece[0]) for piece in pair_pieces(k, chunks)]
        keys += [("next", k), ("last", k)]
    return {key: place for place, key in enumerate(keys)}


def kernel(
    n,
    offset_ref,
    ids_hbm,
    gate_hbm,
    x_hbm,
    w_hbm,
    out_ref,
    ids,
    gates,
    x,
    w,
    outg,
    recv,
    lhs,
    own,
    psend,
    crecv,
    ysend,
    yrecv,
    zsend,
    zrecv,
    zlast,
    sems,
    side_ready,
    ready,
):
    me = lax.axis_index("ep")
    features, width = w.shape
    chunks, _, part, _ = recv.shape
    chosen = ids.shape[0]
    pairs = part * chosen
    rows_all = n * part
    groups = n // 4
    half = n // 2
    line_at = me // 4
    at_end = jnp.logical_or(line_at == 0, line_at == groups - 1)
    inside = jnp.logical_not(at_end)
    plan = semaphore_plan(chunks, groups)

    def sem(*key):
        return sems.at[plan[key if len(key) > 1 else key[0]]]

    def remote(src, dst, send_sem, recv_sem, distance):
        return pltpu.make_async_remote_copy(
            src_ref=src,
            dst_ref=dst,
            send_sem=send_sem,
            recv_sem=recv_sem,
            device_id={"ep": flipped(me, distance)},
            device_id_type=MESH,
        )

    def local(src, dst, key):
        copy = pltpu.make_async_copy(src, dst, sem(key))
        copy.start()
        return copy

    def tell(semaphore, distance):
        pl.semaphore_signal(
            semaphore, inc=1, device_id={"ep": flipped(me, distance)}, device_id_type=MESH
        )

    barrier = pltpu.get_barrier_semaphore()
    for d in range(1, 6):
        tell(barrier, d)

    @pl.when(inside)
    def _():
        for d in (6, 7, 12, 13):
            tell(barrier, d)

    ids_copy = local(ids_hbm, ids, "ids")
    gates_copy = local(gate_hbm, gates, "gates")
    first, later = pl.ds(0, part), pl.ds(part, (chunks - 1) * part)
    x_first = local(x_hbm.at[first], x.at[first], "x_first")
    x_rest = local(x_hbm.at[later], x.at[later], "x_rest")
    w_copy = local(w_hbm.at[0], w, "w")

    slots = [slot_distance(n, s) for s in range(n)]
    others = [s for s, d in enumerate(slots) if d]
    peers = [flipped(me, d) for d in slots]
    lane = lax.broadcasted_iota(jnp.int32, (chosen, pairs), 1)
    spread = (lane % chosen == lax.broadcasted_iota(jnp.int32, (chosen, pairs), 0)).astype(jnp.bfloat16)
    mine = (
        lax.broadcasted_iota(jnp.int32, (rows_all, pairs), 1) // chosen
        == lax.broadcasted_iota(jnp.int32, (rows_all, pairs), 0) % part
    )
    peer_of = jnp.concatenate([jnp.full((part, chosen), e, jnp.int32) for e in peers], axis=0).astype(
        jnp.float32
    )

    dispatch = {}
    for k in range(chunks):
        for place, s in enumerate(others):
            dispatch[k, slots[s]] = remote(
                outg.at[k, place], recv.at[k, s], sem("dispatch_out"), sem("dispatch", k), slots[s]
            )

    straight, turning = (0, 1), (2, 3)

    def issue(k, lines, lows=turning + straight):
        if k < chunks:
            for dz in lines:
                for low in lows:
                    if dz * 4 + low:
                        dispatch[k, dz * 4 + low].start()

    far = tuple(range(groups - 1, 1, -1))

    def issue_early(k):
        issue(k, (0,))

        @pl.when(inside)
        def _():
            if k == 0:
                tell(side_ready, 2)
                issue(0, (3, 1), straight)
            elif k == 1:
                issue(1, (3,), straight)
                pl.semaphore_wait(side_ready, 1)
                tell(ready, 4)
                tell(ready, 12)
                issue(0, (3, 1), turning)
                pl.semaphore_wait(ready, 1)
                tell(ready, 4)
                issue(0, (2,))
                issue(1, (3,), turning)
                issue(1, (2, 1))
            else:
                issue(k, (1,) if k > AHEAD else far + (1,))

        @pl.when(at_end)
        def _():
            if k == 1:
                pl.semaphore_wait(ready, 2)
            if 0 < k <= LEAD:
                issue(k - 1, far)
            if k < LEAD + 2:
                issue(k, (1,))

    def issue_late(k):
        @pl.when(inside)
        def _():
            if k + AHEAD + 1 < chunks:
                issue(k + AHEAD + 1, far)

        @pl.when(at_end)
        def _():
            issue(k + LEAD + 2, (1,))
            issue(k + LEAD, far)

    ids_copy.wait()
    gates_copy.wait()
    target_all = lax.rem(ids[...] - offset_ref[0] + n, n).astype(jnp.float32).T
    gates_all = gates[...].T

    def prepare(k):
        target = target_all[k * part : (k + 1) * part]
        weight = gates_all[k * part : (k + 1) * part]
        hit = jnp.where(jnp.concatenate([target] * n, axis=0) == peer_of, 1.0, 0.0)
        scale = jnp.sum(hit * jnp.concatenate([weight] * n, axis=0), axis=1, keepdims=True)
        wanted = jnp.dot(hit.astype(jnp.bfloat16), spread, preferred_element_type=jnp.float32)
        pick = jnp.where(mine, wanted, 0.0).astype(jnp.bfloat16)
        if k == 0:
            x_first.wait()
        if k == 1:
            x_rest.wait()
        for c in range(0, features, TILE):
            gate = x[k * part : (k + 1) * part, :, c : c + TILE].astype(jnp.float32)
            upper = x[k * part : (k + 1) * part, :, features + c : features + c + TILE].astype(jnp.float32)
            hidden = (jax.nn.silu(gate) * upper).reshape(pairs, TILE).astype(jnp.bfloat16)
            rows = jnp.dot(pick, hidden, preferred_element_type=jnp.float32)
            rows = (rows * scale).reshape(n, part, TILE).astype(jnp.bfloat16)
            for s, d in enumerate(slots):
                if d:
                    outg[k, others.index(s), :, c : c + TILE] = rows[s]
                else:
                    recv[k, s, :, c : c + TILE] = rows[s]

    for k in range(chunks):
        prepare(k)
        if k == 0:
            pl.semaphore_wait(barrier, 7)
        issue_early(k)
    w_copy.wait()

    core, side = {}, {}

    def multiply(k):
        remote(
            outg.at[k], recv.at[k, pl.ds(0, n - 1)], sem("dispatch_out"), sem("dispatch", k), 1
        ).wait_recv()
        issue_late(k)
        lhs[...] = recv[k].astype(jnp.float32).reshape(rows_all, features).astype(jnp.bfloat16)
        parts = core_parts(k, chunks)
        span = width // parts
        for h in range(parts):

            @pl.loop(0, span // COLUMNS)
            def _(j):
                here = pl.ds(pl.multiple_of(h * span + j * COLUMNS, 128), COLUMNS)
                result = jnp.dot(lhs[...], w[:, here], preferred_element_type=jnp.float32)
                result = result.reshape(n, part, COLUMNS)
                own[k, :, :, here] = result[:half]
                psend[k, :, :, here] = result[half:].astype(jnp.bfloat16)

            cols = pl.ds(h * span, span)
            core[k, h] = remote(
                psend.at[k, :, :, cols], crecv.at[k, :, :, cols], sem("core_out"), sem("core", k, h), 1
            )
            core[k, h].start()

    def summed(k, s):
        return own[k, s] + crecv[k, s].astype(jnp.float32)

    def at_dz(dz):
        return groups - 1 - dz

    def send_side(k, piece):
        here = pl.ds(at_dz(piece[0]), len(piece))
        side[k, piece[0]] = remote(
            ysend.at[k, here], yrecv.at[k, here], sem("side_out"), sem("side", k, piece[0]), 2
        )
        side[k, piece[0]].start()

    def finish_core(k):
        for h in range(core_parts(k, chunks)):
            core[k, h].wait_recv()
        for piece in side_pieces(k, chunks, groups):
            for dz in piece:
                ysend[k, at_dz(dz)] = summed(k, groups + at_dz(dz)).astype(jnp.bfloat16)
            if piece != [0]:
                send_side(k, piece)

    def finish_core_later(k):
        if [0] in side_pieces(k, chunks, groups):
            send_side(k, [0])

    def need_side(k, members):
        for piece in side_pieces(k, chunks, groups):
            if (k, piece[0]) in side and set(piece) & set(members):
                side.pop((k, piece[0])).wait_recv()

    def value_of(k, dz):
        return summed(k, at_dz(dz)) + yrecv[k, at_dz(dz)].astype(jnp.float32)

    def line_copy(kind, k, here, landing, distance):
        return remote(zsend.at[k, here], landing, sem("line_out"), sem(kind, k), distance)

    def pair_copy(k, piece):
        here = pl.ds(at_dz(piece[0]), len(piece))
        return remote(zsend.at[k, here], zrecv.at[k, here], sem("line_out"), sem("pair", k, piece[0]), 4)

    one = pl.ds(2, 1)

    def pass_copy(k, dz):
        return line_copy("last", k, pl.ds(at_dz(dz), 1), zlast.at[pl.ds(k, 1)], 4 * dz)


    def start_line(k):
        for piece in pair_pieces(k, chunks):
            need_side(k, piece)

            @pl.when(at_end)
            def _():
                for dz in piece:
                    zsend[k, at_dz(dz)] = value_of(k, dz).astype(jnp.bfloat16)
                pair_copy(k, piece).start()

        need_side(k, (1,))
        zsend[k, at_dz(1)] = value_of(k, 1).astype(jnp.bfloat16)

        @pl.when(jnp.logical_or(inside, k < chunks - HOLD))
        def _():
            line_copy("next", k, one, zrecv.at[k, one], 4).start()

    def send_held(k):
        @pl.when(at_end)
        def _():
            line_copy("next", k, one, zrecv.at[k, one], 4).start()

    def pass_line(k):
        @pl.when(inside)
        def _():
            for piece in pair_pieces(k, chunks):
                pair_copy(k, piece).wait_recv()
                for landed in piece:
                    dz = 5 - landed
                    added = zrecv[k, at_dz(landed)].astype(jnp.float32)
                    zsend[k, at_dz(dz)] = (value_of(k, dz) + added).astype(jnp.bfloat16)
                    if dz == 2 or k < chunks - SKIP:
                        pass_copy(k, dz).start()

    def pass_held(k):
        @pl.when(inside)
        def _():
            pass_copy(k, 3).start()

    def finish(k):
        need_side(k, (0,))
        line_copy("next", k, one, zrecv.at[k, one], 4).wait_recv()
        value = value_of(k, 0) + zrecv[k, at_dz(1)].astype(jnp.float32)
        line_copy("last", k, one, zlast.at[pl.ds(k, 1)], 4).wait_recv()
        out_ref[k] = (value + zlast[k].astype(jnp.float32)).astype(jnp.bfloat16)

    events = []
    last_at = FIRST + TURN * (chunks - 1)
    for k in range(chunks):
        at = FIRST + TURN * k
        events.append((at, k, multiply))
        events.append((at + 2.5, k, finish_core))
        events.append((last_at + 2.55, k, finish_core_later))
        events.append((at + Y_LAG, k, start_line))
        if k >= chunks - HOLD:
            events.append((last_at + Y_LAG + 0.01, k, send_held))
        events.append((at + Y_LAG + Z_LAG, k, pass_line))
        if k >= chunks - SKIP:
            events.append((last_at + Y_LAG + Z_LAG + 0.01, k, pass_held))
        events.append((EARLY if k < chunks - DEFER else LATE, k, finish))
    for _, k, step in sorted(events, key=lambda event: event[:2]):
        step(k)
    for buffer, key in (
        (outg, "dispatch_out"),
        (psend, "core_out"),
        (ysend, "side_out"),
        (zsend, "line_out"),
    ):
        remote(buffer, buffer, sem(key), sem(key), 1).wait_send()


def scratch_of(n, tokens, chosen, features, width):
    chunks = tokens // PART
    groups, half = n // 4, n // 2
    small = jnp.bfloat16
    return [
        ((chosen, tokens), jnp.int32),
        ((chosen, tokens), jnp.float32),
        ((tokens, chosen, 2 * features), small),
        ((features, width), small),
        ((chunks, n - 1, PART, features), small),
        ((chunks, n, PART, features), small),
        ((n * PART, features), small),
        ((chunks, half, PART, width), jnp.float32),
        ((chunks, half, PART, width), small),
        ((chunks, half, PART, width), small),
        ((chunks, groups, PART, width), small),
        ((chunks, groups, PART, width), small),
        ((chunks, groups - 1, PART, width), small),
        ((chunks, groups - 1, PART, width), small),
        ((chunks, PART, width), small),
    ]


def bytes_of(buffers):
    total = 0
    for shape, kind in buffers:
        size = jnp.dtype(kind).itemsize
        for extent in shape:
            size *= extent
        total += size
    return total


def on_device(expert_ids, route_gates, routed_in, down_weight, slot_offset):
    n = lax.axis_size("ep")
    tokens, chosen = expert_ids.shape
    features, width = down_weight.shape[1:]
    buffers = scratch_of(n, tokens, chosen, features, width)
    if (
        n != 16
        or tokens % PART
        or tokens < 4 * PART
        or chosen % 8
        or features % TILE
        or width % (2 * COLUMNS)
        or bytes_of(buffers) > VMEM_LIMIT * 7 // 8
    ):
        return exchange_form(expert_ids, route_gates, routed_in, down_weight, slot_offset)
    chunks, groups = tokens // PART, n // 4
    in_hbm = [
        pltpu.with_memory_space_constraint(array, pltpu.HBM)
        for array in (expert_ids.T, route_gates.T, routed_in, down_weight)
    ]
    result = pl.pallas_call(
        functools.partial(kernel, n),
        out_shape=jax.ShapeDtypeStruct((chunks, PART, width), jnp.bfloat16),
        in_specs=[pl.BlockSpec(memory_space=pltpu.SMEM)] + [pl.BlockSpec(memory_space=pltpu.HBM)] * 4,
        out_specs=pl.BlockSpec(memory_space=pltpu.VMEM),
        scratch_shapes=[pltpu.VMEM(shape, kind) for shape, kind in buffers]
        + [pltpu.SemaphoreType.DMA((len(semaphore_plan(chunks, groups)),)), pltpu.SemaphoreType.REGULAR, pltpu.SemaphoreType.REGULAR],
        compiler_params=pltpu.CompilerParams(
            collective_id=0, has_side_effects=True, vmem_limit_bytes=VMEM_LIMIT
        ),
    )(slot_offset, *in_hbm)
    return result.reshape(tokens, width)


def solution(mesh):
    placed = (
        P(("grp", "ep"), None),
        P(("grp", "ep"), None),
        P(("grp", "ep"), None, None),
        P("ep", None, None),
        P(),
    )
    return jax.shard_map(
        on_device, mesh=mesh, in_specs=placed, out_specs=P(("grp", "ep"), None), check_vma=False
    )
```

```python
import functools

import jax
import jax.numpy as jnp
from jax import lax
from jax.experimental import pallas as pl
from jax.experimental.pallas import tpu as pltpu
from jax.sharding import PartitionSpec as P

MESH = pl.DeviceIdType.MESH
TILE = 256
COLUMNS = 1792
PART = 8
LEAD, AHEAD = 3, 3
FINE, DEFER, HOLD = 2, 5, 4
FIRST, TURN = 8.0, 6.2
Y_LAG, Z_LAG = 15.1, 6.5
SKIP = 2
EARLY, LATE = 54.2, 100.0
VMEM_LIMIT = 48 * 1024 * 1024


def swiglu(packed):
    half = packed.shape[-1] // 2
    gate = packed[..., :half].astype(jnp.float32)
    upper = packed[..., half:].astype(jnp.float32)
    return (jax.nn.silu(gate) * upper).astype(jnp.bfloat16)


def exchange_form(expert_ids, route_gates, routed_in, down_weight, slot_offset):
    experts = lax.axis_size("ep")
    tokens_here, chosen = expert_ids.shape
    pair_count = tokens_here * chosen
    capacity = 2 * pair_count // experts
    matrix = down_weight[0]
    offset = slot_offset[0]
    target = jnp.mod(expert_ids.reshape(pair_count) - offset, experts)
    onehot = (target[:, None] == jnp.arange(experts, dtype=jnp.int32)[None, :]).astype(jnp.int32)
    earlier = jnp.cumsum(onehot, axis=0) - onehot
    rank = jnp.sum(earlier * onehot, axis=1)
    row_index = target * capacity + rank
    source = (
        jnp.full((experts * capacity,), pair_count, jnp.int32)
        .at[row_index]
        .set(jnp.arange(pair_count, dtype=jnp.int32))
    )
    payload = swiglu(routed_in.reshape(pair_count, routed_in.shape[2]))
    padded = jnp.concatenate([payload, jnp.zeros((1, payload.shape[1]), jnp.bfloat16)], axis=0)
    outgoing = jnp.take(padded, source, axis=0).reshape(experts, capacity, payload.shape[1])
    results = jnp.einsum(
        "nkf,fd->nkd",
        lax.all_to_all(outgoing, "ep", split_axis=0, concat_axis=0, tiled=True),
        matrix,
        preferred_element_type=jnp.float32,
    ).astype(jnp.bfloat16)
    returned = lax.all_to_all(results, "ep", split_axis=0, concat_axis=0, tiled=True)
    width = returned.shape[2]
    picked = jnp.take(returned.reshape(experts * capacity, width), row_index, axis=0).reshape(
        tokens_here, chosen, width
    )
    total = jnp.zeros((tokens_here, width), jnp.float32)
    for choice_index in range(chosen):
        total = total + route_gates[:, choice_index, None] * picked[:, choice_index].astype(
            jnp.float32
        )
    return total.astype(jnp.bfloat16)


def flipped(index, distance):
    result, bit = index, 1
    while bit <= distance:
        if distance & bit:
            result = result + bit - 2 * bit * lax.rem(lax.div(index, bit), 2)
        bit *= 2
    return result


def slot_distance(n, slot):
    groups = n // 4
    return (groups - 1 - slot % groups) * 4 + (slot // groups % 2) * 2 + slot // (2 * groups)


def is_fine(k, chunks):
    return k >= chunks - FINE


def core_parts(k, chunks):
    return 2 if is_fine(k, chunks) else 1


def side_pieces(k, chunks, groups):
    sums = list(range(groups - 1, -1, -1))
    if is_fine(k, chunks):
        return [[dz] for dz in sums]
    return [sums[:-1], sums[-1:]] if k >= chunks - DEFER else [sums]


def pair_pieces(k, chunks):
    return [[3], [2]] if is_fine(k, chunks) else [[3, 2]]


def semaphore_plan(chunks, groups):
    keys = ["w", "ids", "gates", "x_first", "x_rest", "dispatch_out", "core_out", "side_out", "line_out"]
    for k in range(chunks):
        keys.append(("dispatch", k))
        keys += [("core", k, h) for h in range(core_parts(k, chunks))]
        keys += [("side", k, piece[0]) for piece in side_pieces(k, chunks, groups)]
        keys += [("pair", k, piece[0]) for piece in pair_pieces(k, chunks)]
        keys += [("next", k), ("last", k)]
    return {key: place for place, key in enumerate(keys)}


def kernel(
    n,
    offset_ref,
    ids_hbm,
    gate_hbm,
    x_hbm,
    w_hbm,
    out_ref,
    ids,
    gates,
    x,
    w,
    outg,
    recv,
    lhs,
    own,
    psend,
    crecv,
    ysend,
    yrecv,
    zsend,
    zrecv,
    zlast,
    sems,
    side_ready,
    ready,
):
    me = lax.axis_index("ep")
    features, width = w.shape
    chunks, _, part, _ = recv.shape
    chosen = ids.shape[0]
    pairs = part * chosen
    rows_all = n * part
    groups = n // 4
    half = n // 2
    line_at = me // 4
    at_end = jnp.logical_or(line_at == 0, line_at == groups - 1)
    inside = jnp.logical_not(at_end)
    plan = semaphore_plan(chunks, groups)

    def sem(*key):
        return sems.at[plan[key if len(key) > 1 else key[0]]]

    def remote(src, dst, send_sem, recv_sem, distance):
        return pltpu.make_async_remote_copy(
            src_ref=src,
            dst_ref=dst,
            send_sem=send_sem,
            recv_sem=recv_sem,
            device_id={"ep": flipped(me, distance)},
            device_id_type=MESH,
        )

    def local(src, dst, key):
        copy = pltpu.make_async_copy(src, dst, sem(key))
        copy.start()
        return copy

    def tell(semaphore, distance):
        pl.semaphore_signal(
            semaphore, inc=1, device_id={"ep": flipped(me, distance)}, device_id_type=MESH
        )

    barrier = pltpu.get_barrier_semaphore()
    for d in range(1, 6):
        tell(barrier, d)

    @pl.when(inside)
    def _():
        for d in (6, 7, 12, 13):
            tell(barrier, d)

    ids_copy = local(ids_hbm, ids, "ids")
    gates_copy = local(gate_hbm, gates, "gates")
    first, later = pl.ds(0, part), pl.ds(part, (chunks - 1) * part)
    x_first = local(x_hbm.at[first], x.at[first], "x_first")
    x_rest = local(x_hbm.at[later], x.at[later], "x_rest")
    w_copy = local(w_hbm.at[0], w, "w")

    slots = [slot_distance(n, s) for s in range(n)]
    others = [s for s, d in enumerate(slots) if d]
    peers = [flipped(me, d) for d in slots]
    lane = lax.broadcasted_iota(jnp.int32, (chosen, pairs), 1)
    spread = (lane % chosen == lax.broadcasted_iota(jnp.int32, (chosen, pairs), 0)).astype(jnp.bfloat16)
    mine = (
        lax.broadcasted_iota(jnp.int32, (rows_all, pairs), 1) // chosen
        == lax.broadcasted_iota(jnp.int32, (rows_all, pairs), 0) % part
    )
    peer_of = jnp.concatenate([jnp.full((part, chosen), e, jnp.int32) for e in peers], axis=0).astype(
        jnp.float32
    )

    dispatch = {}
    for k in range(chunks):
        for place, s in enumerate(others):
            dispatch[k, slots[s]] = remote(
                outg.at[k, place], recv.at[k, s], sem("dispatch_out"), sem("dispatch", k), slots[s]
            )

    straight, turning = (0, 1), (2, 3)

    def issue(k, lines, lows=turning + straight):
        if k < chunks:
            for dz in lines:
                for low in lows:
                    if dz * 4 + low:
                        dispatch[k, dz * 4 + low].start()

    far = tuple(range(2, groups))

    def issue_early(k):
        issue(k, (0,))

        @pl.when(inside)
        def _():
            if k == 0:
                tell(side_ready, 2)
                issue(0, (3, 1), straight)
            elif k == 1:
                issue(1, (3,), straight)
                pl.semaphore_wait(side_ready, 1)
                tell(ready, 4)
                tell(ready, 12)
                issue(0, (3, 1), turning)
                pl.semaphore_wait(ready, 1)
                tell(ready, 4)
                issue(0, (2,))
                issue(1, (3,), turning)
                issue(1, (2, 1))
            else:
                issue(k, (1,) if k > AHEAD else far + (1,))

        @pl.when(at_end)
        def _():
            if k == 1:
                pl.semaphore_wait(ready, 2)
            if 0 < k <= LEAD:
                issue(k - 1, far)
            if k < LEAD + 2:
                issue(k, (1,))

    def issue_late(k):
        @pl.when(inside)
        def _():
            if k + AHEAD + 1 < chunks:
                issue(k + AHEAD + 1, far)

        @pl.when(at_end)
        def _():
            issue(k + LEAD + 2, (1,))
            issue(k + LEAD, far)

    ids_copy.wait()
    gates_copy.wait()
    target_all = lax.rem(ids[...] - offset_ref[0] + n, n).astype(jnp.float32).T
    gates_all = gates[...].T

    def prepare(k):
        target = target_all[k * part : (k + 1) * part]
        weight = gates_all[k * part : (k + 1) * part]
        hit = jnp.where(jnp.concatenate([target] * n, axis=0) == peer_of, 1.0, 0.0)
        scale = jnp.sum(hit * jnp.concatenate([weight] * n, axis=0), axis=1, keepdims=True)
        wanted = jnp.dot(hit.astype(jnp.bfloat16), spread, preferred_element_type=jnp.float32)
        pick = jnp.where(mine, wanted, 0.0).astype(jnp.bfloat16)
        if k == 0:
            x_first.wait()
        if k == 1:
            x_rest.wait()
        for c in range(0, features, TILE):
            gate = x[k * part : (k + 1) * part, :, c : c + TILE].astype(jnp.float32)
            upper = x[k * part : (k + 1) * part, :, features + c : features + c + TILE].astype(jnp.float32)
            hidden = (jax.nn.silu(gate) * upper).reshape(pairs, TILE).astype(jnp.bfloat16)
            rows = jnp.dot(pick, hidden, preferred_element_type=jnp.float32)
            rows = (rows * scale).reshape(n, part, TILE).astype(jnp.bfloat16)
            for s, d in enumerate(slots):
                if d:
                    outg[k, others.index(s), :, c : c + TILE] = rows[s]
                else:
                    recv[k, s, :, c : c + TILE] = rows[s]

    for k in range(chunks):
        prepare(k)
        if k == 0:
            pl.semaphore_wait(barrier, 7)
        issue_early(k)
    w_copy.wait()

    core, side = {}, {}

    def multiply(k):
        remote(
            outg.at[k], recv.at[k, pl.ds(0, n - 1)], sem("dispatch_out"), sem("dispatch", k), 1
        ).wait_recv()
        issue_late(k)
        lhs[...] = recv[k].astype(jnp.float32).reshape(rows_all, features).astype(jnp.bfloat16)
        parts = core_parts(k, chunks)
        span = width // parts
        for h in range(parts):

            @pl.loop(0, span // COLUMNS)
            def _(j):
                here = pl.ds(pl.multiple_of(h * span + j * COLUMNS, 128), COLUMNS)
                result = jnp.dot(lhs[...], w[:, here], preferred_element_type=jnp.float32)
                result = result.reshape(n, part, COLUMNS)
                own[k, :, :, here] = result[:half]
                psend[k, :, :, here] = result[half:].astype(jnp.bfloat16)

            cols = pl.ds(h * span, span)
            core[k, h] = remote(
                psend.at[k, :, :, cols], crecv.at[k, :, :, cols], sem("core_out"), sem("core", k, h), 1
            )
            core[k, h].start()

    def summed(k, s):
        return own[k, s] + crecv[k, s].astype(jnp.float32)

    def at_dz(dz):
        return groups - 1 - dz

    def send_side(k, piece):
        here = pl.ds(at_dz(piece[0]), len(piece))
        side[k, piece[0]] = remote(
            ysend.at[k, here], yrecv.at[k, here], sem("side_out"), sem("side", k, piece[0]), 2
        )
        side[k, piece[0]].start()

    def finish_core(k):
        for h in range(core_parts(k, chunks)):
            core[k, h].wait_recv()
        for piece in side_pieces(k, chunks, groups):
            for dz in piece:
                ysend[k, at_dz(dz)] = summed(k, groups + at_dz(dz)).astype(jnp.bfloat16)
            if piece != [0]:
                send_side(k, piece)

    def finish_core_later(k):
        if [0] in side_pieces(k, chunks, groups):
            send_side(k, [0])

    def need_side(k, members):
        for piece in side_pieces(k, chunks, groups):
            if (k, piece[0]) in side and set(piece) & set(members):
                side.pop((k, piece[0])).wait_recv()

    def value_of(k, dz):
        return summed(k, at_dz(dz)) + yrecv[k, at_dz(dz)].astype(jnp.float32)

    def line_copy(kind, k, here, landing, distance):
        return remote(zsend.at[k, here], landing, sem("line_out"), sem(kind, k), distance)

    def pair_copy(k, piece):
        here = pl.ds(at_dz(piece[0]), len(piece))
        return remote(zsend.at[k, here], zrecv.at[k, here], sem("line_out"), sem("pair", k, piece[0]), 4)

    one = pl.ds(2, 1)

    def pass_copy(k, dz):
        return line_copy("last", k, pl.ds(at_dz(dz), 1), zlast.at[pl.ds(k, 1)], 4 * dz)


    def start_line(k):
        for piece in pair_pieces(k, chunks):
            need_side(k, piece)

            @pl.when(at_end)
            def _():
                for dz in piece:
                    zsend[k, at_dz(dz)] = value_of(k, dz).astype(jnp.bfloat16)
                pair_copy(k, piece).start()

        need_side(k, (1,))
        zsend[k, at_dz(1)] = value_of(k, 1).astype(jnp.bfloat16)

        @pl.when(jnp.logical_or(inside, k < chunks - HOLD))
        def _():
            line_copy("next", k, one, zrecv.at[k, one], 4).start()

    def send_held(k):
        @pl.when(at_end)
        def _():
            line_copy("next", k, one, zrecv.at[k, one], 4).start()

    def pass_line(k):
        @pl.when(inside)
        def _():
            for piece in pair_pieces(k, chunks):
                pair_copy(k, piece).wait_recv()
                for landed in piece:
                    dz = 5 - landed
                    added = zrecv[k, at_dz(landed)].astype(jnp.float32)
                    zsend[k, at_dz(dz)] = (value_of(k, dz) + added).astype(jnp.bfloat16)
                    if dz == 2 or k < chunks - SKIP:
                        pass_copy(k, dz).start()

    def pass_held(k):
        @pl.when(inside)
        def _():
            pass_copy(k, 3).start()

    def finish(k):
        need_side(k, (0,))
        line_copy("next", k, one, zrecv.at[k, one], 4).wait_recv()
        value = value_of(k, 0) + zrecv[k, at_dz(1)].astype(jnp.float32)
        line_copy("last", k, one, zlast.at[pl.ds(k, 1)], 4).wait_recv()
        out_ref[k] = (value + zlast[k].astype(jnp.float32)).astype(jnp.bfloat16)

    events = []
    last_at = FIRST + TURN * (chunks - 1)
    for k in range(chunks):
        at = FIRST + TURN * k
        events.append((at, k, multiply))
        events.append((at + 2.5, k, finish_core))
        events.append((last_at + 2.55, k, finish_core_later))
        events.append((at + Y_LAG, k, start_line))
        if k >= chunks - HOLD:
            events.append((last_at + Y_LAG + 0.01, k, send_held))
        events.append((at + Y_LAG + Z_LAG, k, pass_line))
        if k >= chunks - SKIP:
            events.append((last_at + Y_LAG + Z_LAG + 0.01, k, pass_held))
        events.append((EARLY if k < chunks - DEFER else LATE, k, finish))
    for _, k, step in sorted(events, key=lambda event: event[:2]):
        step(k)
    for buffer, key in (
        (outg, "dispatch_out"),
        (psend, "core_out"),
        (ysend, "side_out"),
        (zsend, "line_out"),
    ):
        remote(buffer, buffer, sem(key), sem(key), 1).wait_send()


def scratch_of(n, tokens, chosen, features, width):
    chunks = tokens // PART
    groups, half = n // 4, n // 2
    small = jnp.bfloat16
    return [
        ((chosen, tokens), jnp.int32),
        ((chosen, tokens), jnp.float32),
        ((tokens, chosen, 2 * features), small),
        ((features, width), small),
        ((chunks, n - 1, PART, features), small),
        ((chunks, n, PART, features), small),
        ((n * PART, features), small),
        ((chunks, half, PART, width), jnp.float32),
        ((chunks, half, PART, width), small),
        ((chunks, half, PART, width), small),
        ((chunks, groups, PART, width), small),
        ((chunks, groups, PART, width), small),
        ((chunks, groups - 1, PART, width), small),
        ((chunks, groups - 1, PART, width), small),
        ((chunks, PART, width), small),
    ]


def bytes_of(buffers):
    total = 0
    for shape, kind in buffers:
        size = jnp.dtype(kind).itemsize
        for extent in shape:
            size *= extent
        total += size
    return total


def on_device(expert_ids, route_gates, routed_in, down_weight, slot_offset):
    n = lax.axis_size("ep")
    tokens, chosen = expert_ids.shape
    features, width = down_weight.shape[1:]
    buffers = scratch_of(n, tokens, chosen, features, width)
    if (
        n != 16
        or tokens % PART
        or tokens < 4 * PART
        or chosen % 8
        or features % TILE
        or width % (2 * COLUMNS)
        or bytes_of(buffers) > VMEM_LIMIT * 7 // 8
    ):
        return exchange_form(expert_ids, route_gates, routed_in, down_weight, slot_offset)
    chunks, groups = tokens // PART, n // 4
    in_hbm = [
        pltpu.with_memory_space_constraint(array, pltpu.HBM)
        for array in (expert_ids.T, route_gates.T, routed_in, down_weight)
    ]
    result = pl.pallas_call(
        functools.partial(kernel, n),
        out_shape=jax.ShapeDtypeStruct((chunks, PART, width), jnp.bfloat16),
        in_specs=[pl.BlockSpec(memory_space=pltpu.SMEM)] + [pl.BlockSpec(memory_space=pltpu.HBM)] * 4,
        out_specs=pl.BlockSpec(memory_space=pltpu.VMEM),
        scratch_shapes=[pltpu.VMEM(shape, kind) for shape, kind in buffers]
        + [pltpu.SemaphoreType.DMA((len(semaphore_plan(chunks, groups)),)), pltpu.SemaphoreType.REGULAR, pltpu.SemaphoreType.REGULAR],
        compiler_params=pltpu.CompilerParams(
            collective_id=0, has_side_effects=True, vmem_limit_bytes=VMEM_LIMIT
        ),
    )(slot_offset, *in_hbm)
    return result.reshape(tokens, width)


def solution(mesh):
    placed = (
        P(("grp", "ep"), None),
        P(("grp", "ep"), None),
        P(("grp", "ep"), None, None),
        P("ep", None, None),
        P(),
    )
    return jax.shard_map(
        on_device, mesh=mesh, in_specs=placed, out_specs=P(("grp", "ep"), None), check_vma=False
    )
```
